1024 devices in a mesh: slab: 2 (over core), py: 16 (over z), pz: 32 (over x, y).
Axes of the slice: x: 4, y: 8, z: 16, core: 2. Of those that a mesh axis runs over, the one named last changes fastest.
Arguments:
- start_vector: float32 [256, 512, 256], P('pz', 'py', 'slab'), may hold values from -6 to 6
- potential: float32 [256, 512, 256], P('pz', 'py', 'slab'), may hold values from 0.5 to 4
Outputs:
- krylov_basis: float32 [6, 256, 512, 256], P(None, 'pz', 'py', 'slab')
- tridiagonal: float32 [2, 5], replicated
The draws below stay inside these ranges and needn't reach their ends.
All inputs are finite; a program needn't handle non-finite values.
Results may differ from the reference program's by a relative error of at most 0.00012.
Values sent between devices are 32-bit elements; how exact they have to be, the bound alone decides.
No kernel may reach another device: no remote copies, remote signals or barrier semaphores. Data moves between devices by JAX's collectives and lax.ppermute only.
A program may use at most 32 MiB of HBM per device.

```python
import jax
import jax.numpy as jnp
from jax import lax

ITERS = 5
NX = 256
NY = 512
NZ = 256


def level_of(key, dims, shards, smallest, top_value):
    loudness = 1.0
    for position, parts in shards:
        steps = jax.random.uniform(jax.random.fold_in(jax.random.fold_in(key, 6), position), (parts,), jnp.float32, smallest / len(shards), top_value / len(shards))
        loudness = loudness * jnp.repeat(jnp.exp(steps), dims[position] // parts).reshape((-1,) + (1,) * (len(dims) - 1 - position))
    return loudness


def normal_values(key, shape, deviation, limit, split=(), dtype=jnp.bfloat16):
    values = jax.random.normal(key, shape, jnp.float32) * deviation
    if len(split) > 0:
        values = level_of(key, shape, split, -0.22, 0.18) * values
    return jnp.clip(values, min=-limit, max=limit).astype(dtype)


def setup_inputs(seed: int = 0) -> dict:
    key_of = jax.random.split(jax.random.key(seed), 3)
    return {
        "start_vector": normal_values(key_of[0], (NZ, NY, NX), 1.0, 6.0, ((0, 32), (1, 16), (2, 2)), jnp.float32),
        "potential": jnp.clip(0.5 + 3.5 * jax.random.uniform(key_of[1], (NZ, NY, NX), jnp.float32) ** level_of(key_of[1], (NZ, NY, NX), ((0, 32), (1, 16), (2, 2)), -0.2, 0.2), 0.5, 4.0),
    }


EPSILON = 1e-06

def apply_hamiltonian(field, potential):
    padded = jnp.pad(field, 1)
    beside = padded[2:, 1:-1, 1:-1] + padded[:-2, 1:-1, 1:-1]
    beside = beside + padded[1:-1, 2:, 1:-1] + padded[1:-1, :-2, 1:-1]
    beside = beside + padded[1:-1, 1:-1, 2:] + padded[1:-1, 1:-1, :-2]
    return (6.0 + potential) * field - beside

def reference(start_vector, potential):
    per_cell = jnp.float32(1.0 / (NX * NY * NZ))
    start_norm = jnp.sum(start_vector * start_vector) * per_cell
    vectors = [start_vector / jnp.sqrt(start_norm + EPSILON)]
    alphas = []
    beta_list = []
    for iteration in range(ITERS):
        image = apply_hamiltonian(vectors[-1], potential)
        active = jnp.stack(vectors)
        first_coeff = jnp.einsum('kzyx,zyx->k', active, image, precision=lax.Precision.HIGHEST) * per_cell
        image = image - jnp.einsum('k,kzyx->zyx', first_coeff, active, precision=lax.Precision.HIGHEST)
        second_coeff = jnp.einsum('kzyx,zyx->k', active, image, precision=lax.Precision.HIGHEST) * per_cell
        image = image - jnp.einsum('k,kzyx->zyx', second_coeff, active, precision=lax.Precision.HIGHEST)
        square_mean = jnp.sum(image * image) * per_cell
        beta_value = jnp.sqrt(square_mean + EPSILON)
        alphas.append(first_coeff[iteration] + second_coeff[iteration])
        beta_list.append(beta_value)
        vectors.append(image / beta_value)
    return (jnp.stack(vectors), jnp.stack([jnp.stack(alphas), jnp.stack(beta_list)]))
```

```python
import functools

import jax
import jax.numpy as jnp
from jax import lax
from jax.experimental import pallas as pl
from jax.experimental.pallas import tpu as pltpu
from jax.sharding import PartitionSpec as P

ITERS = 5
EPSILON = 1e-06
INTERPRET = False

SHIFTS = (2.25, 14.25, 8.25, 2.25, 14.25)
SCALE = 2.0**40
COUNT = ITERS + 1
PAIRS = [(i, k) for i in range(COUNT) for k in range(i, COUNT)]
EDGE = 8


def two_sum(a, b):
    s = a + b
    t = s - a
    return s, (a - (s - t)) + (b - t)


def split(a):
    c = a * 4097.0
    high = c - (c - a)
    return high, a - high


def pair_add(a, b):
    s, e = two_sum(a[0], b[0])
    e = e + (a[1] + b[1])
    high = s + e
    return high, e - (high - s)


def pair_mul(a, b):
    p = a[0] * b[0]
    ah, al = split(a[0])
    bh, bl = split(b[0])
    e = ((ah * bh - p) + (ah * bl + al * bh)) + al * bl
    e = e + (a[0] * b[1] + a[1] * b[0])
    high = p + e
    return high, e - (high - p)


def pair_neg(a):
    return -a[0], -a[1]


def pair_sum(terms):
    terms = list(terms)
    while len(terms) > 1:
        rest = terms[len(terms) // 2 * 2 :]
        terms = [pair_add(terms[i], terms[i + 1]) for i in range(0, len(terms) - 1, 2)] + rest
    return terms[0]


def over_sublanes(a):
    for shift in (4, 2, 1):
        a = pair_add(a, (pltpu.roll(a[0], shift, 0), pltpu.roll(a[1], shift, 0)))
    return a


def lanes():
    return lax.broadcasted_iota(jnp.int32, (8, 128), 1)


def as_row(a):
    return jnp.where(lanes() < 64, a[0], pltpu.roll(a[1], 64, 1))


def sum_of_rows(ref):
    blocks = [ref[pl.ds(8 * r, 8), :] for r in range(ref.shape[0] // 8)]
    return over_sublanes(pair_sum([(b, pltpu.roll(b, 64, 1)) for b in blocks]))


def assemble(x, k0, dg, slot):
    depth, height = ITERS, 32

    def put(ref, planes, rows, first, factor):
        n, r = planes.stop - planes.start, rows.stop - rows.start
        piece = x[pl.ds(first, n * r), :].reshape(n, r, 128)
        ref[slot, planes, rows, :] = piece * factor
        return first + n * r

    low, own, high = slice(0, 8), slice(8, 40), slice(40, 48)
    at = put(k0, slice(5, 13), own, 0, SCALE)
    at = put(dg, slice(4, 12), own, at, 0.125)
    for rows in (low, high):
        at = put(k0, slice(5, 13), rows, at, SCALE)
        at = put(dg, slice(4, 12), rows, at, 0.125)
    for side in (0, 1):
        at = put(k0, slice(13, 18) if side else slice(0, 5), own, at, SCALE)
        at = put(dg, slice(12, 16) if side else slice(0, 4), own, at, 0.125)
        for rows in (low, high):
            at = put(k0, slice(13, 17) if side else slice(1, 5), rows, at, SCALE)
        for rows in (low, high):
            at = put(dg, slice(12, 15) if side else slice(1, 4), rows, at, 0.125)
    for rows in (low, high):
        for plane in (0, 17):
            k0[slot, plane, rows, :] = jnp.zeros((8, 128), jnp.float32)
        for plane in (0, 15):
            dg[slot, plane, rows, :] = jnp.zeros((8, 128), jnp.float32)


def krylov_kernel(x, q, k_out, row_out, k0, k1, k2, k3, k4, k5, dg):
    mine = lax.axis_index("slab")
    y, z = lax.axis_index("py"), lax.axis_index("pz")
    inside = {
        "y_low": jnp.where(y > 0, 1.0, 0.0),
        "y_high": jnp.where(y < lax.axis_size("py") - 1, 1.0, 0.0),
        "z_low": jnp.where(z > 0, 1.0, 0.0),
        "z_high": jnp.where(z < lax.axis_size("pz") - 1, 1.0, 0.0),
    }
    assemble(x, k0, dg, mine)
    assemble(q, k0, dg, 1 - mine)
    lane = lax.broadcasted_iota(jnp.int32, (48, 128), 1)
    first, last = lane == 0, lane == 127
    basis = (k0, k1, k2, k3, k4, k5)
    for step in range(1, COUNT):
        old, new = basis[step - 1], basis[step]
        shift = (6.0 - SHIFTS[step - 1]) * 0.125
        for plane in range(step, 18 - step):
            f = [old[t, plane] for t in (0, 1)]
            up = [pltpu.roll(a, 1, 1) for a in f]
            down = [pltpu.roll(a, 127, 1) for a in f]
            beside = [
                jnp.where(first, 0.0, up[0]) + jnp.where(last, down[1], down[0]),
                jnp.where(first, up[0], up[1]) + jnp.where(last, 0.0, down[1]),
            ]
            for t in (0, 1):
                around = beside[t] + (pltpu.roll(f[t], 1, 0) + pltpu.roll(f[t], 47, 0))
                around = around + (old[t, plane - 1] + old[t, plane + 1])
                image = (dg[t, plane - 1] + shift) * f[t] - 0.125 * around
                if step == ITERS:
                    new[t, plane - ITERS] = image[8:40]
                    continue
                if plane < ITERS:
                    image = image * inside["z_low"]
                if plane >= 13:
                    image = image * inside["z_high"]
                new[t, plane, 0:8] = image[0:8] * inside["y_low"]
                new[t, plane, 8:40] = image[8:40]
                new[t, plane, 40:48] = image[40:48] * inside["y_high"]
    sums = [None] * len(PAIRS)
    for plane in range(8):
        for tile in range(4):
            own = [b[mine, 5 + plane, 8 + 8 * tile : 16 + 8 * tile] for b in basis[:ITERS]]
            own.append(k5[mine, plane, 8 * tile : 8 + 8 * tile])
            for i, value in enumerate(own):
                k_out[i, plane, 8 * tile : 8 + 8 * tile] = value
            parts = [split(value) for value in own]
            for n, (i, k) in enumerate(PAIRS):
                big = parts[i][0] * parts[k][0]
                small = parts[i][0] * parts[k][1] + parts[i][1] * own[k]
                if sums[n] is None:
                    sums[n] = (big, small)
                else:
                    s, e = two_sum(sums[n][0], big)
                    sums[n] = (s, sums[n][1] + (e + small))
    row = lax.broadcasted_iota(jnp.int32, (8, 128), 0)
    tables = []
    sums = [over_sublanes(s) for s in sums]
    for half in (0, 1):
        blocks = []
        for start in range(0, len(PAIRS), 8):
            block = sums[start][half]
            for n in range(start + 1, min(start + 8, len(PAIRS))):
                block = jnp.where(row == n - start, sums[n][half], block)
            blocks.append(block)
        blocks.append(jnp.zeros((128 - 8 * len(blocks), 128), jnp.float32))
        tables.append(jnp.transpose(jnp.concatenate(blocks)))
    total = over_sublanes(
        pair_sum([tuple(t[8 * r : 8 * r + 8] for t in tables) for r in range(16)])
    )
    sent = as_row(total)
    for r in range(row_out.shape[0] // 8):
        row_out[8 * r : 8 * r + 8] = sent


def rows_kernel(rows, out):
    sent = as_row(sum_of_rows(rows))
    for r in range(out.shape[0] // 8):
        out[8 * r : 8 * r + 8] = sent


def root_of(square):
    x = pair_add(square, (jnp.full_like(square[0], EPSILON), jnp.zeros_like(square[0])))
    r = lax.rsqrt(x[0])
    for _ in range(2):
        r = r * (1.5 - (0.5 * x[0]) * (r * r))
    zero = jnp.zeros_like(r)
    one = pair_mul(x, pair_mul((r, zero), (r, zero)))
    miss = (1.0 - one[0]) - one[1]
    return x[0] * r, (r, r * (0.5 * miss))


def coefficients(gram):
    zero = jnp.zeros((8, 128), jnp.float32)
    _, inverse = root_of(tuple(g * SCALE**-2 for g in gram[0][0]))
    coeffs = [[tuple(r / SCALE for r in inverse)]]
    lack = [[(EPSILON * inverse[0]) * inverse[0]]]
    alphas, betas = [], []
    for j in range(ITERS):
        newest = coeffs[j]
        image = [None] * (j + 2)
        for i in range(j + 2):
            terms = []
            if i <= j:
                terms.append(pair_mul(newest[i], (jnp.full_like(zero, SHIFTS[i]), zero)))
            if i >= 1:
                terms.append((8.0 * newest[i - 1][0], 8.0 * newest[i - 1][1]))
            image[i] = pair_sum(terms)
        weights = [
            pair_sum([pair_mul(gram[i][k], image[k]) for k in range(j + 2)]) for i in range(j + 2)
        ]
        first = [
            pair_sum([pair_mul(coeffs[k][i], weights[i]) for i in range(k + 1)])
            for k in range(j + 1)
        ]
        second = [sum(lack[k][l] * first[l][0] for l in range(j + 1)) for k in range(j + 1)]
        third = [sum(lack[k][l] * second[l] for l in range(j + 1)) for k in range(j + 1)]
        both = [pair_add(first[k], (second[k], zero)) for k in range(j + 1)]
        rest = sum(
            second[k] * second[k] - both[k][0] * (second[k] + third[k]) for k in range(j + 1)
        )
        square = pair_sum(
            [pair_mul(image[i], weights[i]) for i in range(j + 2)]
            + [pair_neg(pair_mul(f, f)) for f in first]
            + [(rest, zero)]
        )
        positive = square[0] + square[1] > 0.0
        beta, inverse = root_of(tuple(jnp.where(positive, s, 0.0) for s in square))
        alphas.append(both[j][0])
        betas.append(beta)
        following = []
        for i in range(j + 2):
            terms = [image[i]] + [
                pair_neg(pair_mul(both[k], coeffs[k][i])) for k in range(i, j + 1)
            ]
            following.append(pair_mul(pair_sum(terms), inverse))
        coeffs.append(following)
        for k in range(j + 1):
            lack[k].append(-third[k] * inverse[0])
        lack.append([lack[k][j + 1] for k in range(j + 1)] + [(EPSILON * inverse[0]) * inverse[0]])
    return coeffs, alphas, betas


def lanczos_kernel(per_cell, rows, basis, vectors, tridiagonal):
    total = sum_of_rows(rows)
    gram = [[None] * COUNT for _ in range(COUNT)]
    for n, (i, k) in enumerate(PAIRS):
        gram[i][k] = gram[k][i] = tuple(
            jnp.broadcast_to(t[:, n : n + 1], (8, 128)) * per_cell for t in total
        )
    coeffs, alphas, betas = coefficients(gram)
    lane = lanes()
    table = [jnp.zeros((8, 128), jnp.float32)] * 2
    for r, values in enumerate((alphas, betas)):
        for j, value in enumerate(values):
            table[r] = jnp.where(lane == j, value, table[r])
        tridiagonal[r : r + 1, :] = table[r][0:1, 0:ITERS]
    final = [[c[0] + c[1] for c in column] for column in coeffs]
    for plane in range(8):
        for tile in range(4):
            rows_of = slice(8 * tile, 8 * tile + 8)
            k = [basis[i, plane, rows_of] for i in range(COUNT)]
            for j, column in enumerate(final):
                value = column[0] * k[0]
                for i in range(1, j + 1):
                    value = value + column[i] * k[i]
                vectors[j, plane, rows_of] = value


def call(kernel, out_shape, scratch=(), flops=10000, mebibytes=4):
    return pl.pallas_call(
        kernel,
        out_shape=out_shape,
        scratch_shapes=list(scratch),
        cost_estimate=pl.CostEstimate(flops=flops, bytes_accessed=flops, transcendentals=0),
        compiler_params=pltpu.CompilerParams(vmem_limit_bytes=mebibytes * 2**20),
        interpret=INTERPRET,
    )


def to_rows(*pieces):
    return jnp.concatenate([p.reshape(-1, 128) for p in pieces])


def shards(v, p):
    f32 = jnp.float32

    def line(axis, step):
        n = lax.axis_size(axis)
        return [(i, i + step) for i in range(n) if 0 <= i + step < n]

    def exchange(to_next, to_previous, axis):
        return (
            lax.ppermute(to_next, axis, line(axis, 1)),
            lax.ppermute(to_previous, axis, line(axis, -1)),
        )

    last, first = slice(32 - EDGE, 32), slice(0, EDGE)
    y_low, y_high = exchange(
        jnp.stack([v[:, last], p[:, last]]), jnp.stack([v[:, first], p[:, first]]), "py"
    )
    z_low, z_high = exchange(
        to_rows(v[3:], p[4:], y_low[0, 4:], y_high[0, 4:], y_low[1, 5:], y_high[1, 5:]),
        to_rows(v[:5], p[:4], y_low[0, :4], y_high[0, :4], y_low[1, :3], y_high[1, :3]),
        "pz",
    )
    x = to_rows(v, p, y_low, y_high, z_low, z_high)
    q = lax.ppermute(x, "slab", [(0, 1), (1, 0)])
    n_z = lax.axis_size("pz")
    n_xy = lax.axis_size("slab") * lax.axis_size("py")
    block = [pltpu.VMEM((2, 18, 48, 128), f32)] * 5
    basis, rows = call(
        krylov_kernel,
        (jax.ShapeDtypeStruct((COUNT, 8, 32, 128), f32), jax.ShapeDtypeStruct((n_z, 128), f32)),
        block + [pltpu.VMEM((2, 8, 32, 128), f32), pltpu.VMEM((2, 16, 48, 128), f32)],
        20000000,
        12,
    )(x, q)
    rows = lax.all_to_all(rows, "pz", 0, 0, tiled=True)
    rows = call(rows_kernel, jax.ShapeDtypeStruct((n_xy, 128), f32))(rows)
    rows = lax.all_to_all(rows, ("slab", "py"), 0, 0, tiled=True)
    per_cell = 1.0 / (v.size * n_z * n_xy)
    return call(
        functools.partial(lanczos_kernel, per_cell),
        (
            jax.ShapeDtypeStruct((COUNT, 8, 32, 128), f32),
            jax.ShapeDtypeStruct((2, ITERS), f32),
        ),
        flops=20000000,
    )(rows, basis)


def solution(mesh):
    in_specs = (P("pz", "py", "slab"), P("pz", "py", "slab"))
    out_specs = (P(None, "pz", "py", "slab"), P())
    return jax.shard_map(shards, mesh=mesh, in_specs=in_specs, out_specs=out_specs, check_vma=False)
```

```python
import functools

import jax
import jax.numpy as jnp
from jax import lax
from jax.experimental import pallas as pl
from jax.experimental.pallas import tpu as pltpu
from jax.sharding import PartitionSpec as P

ITERS = 5
EPSILON = 1e-06
INTERPRET = False

SHIFTS = (2.25, 14.25, 8.25, 2.25, 14.25)
SCALE = 2.0**24
FIRST = 6.0 - SHIFTS[0]
COUNT = ITERS + 1
PAIRS = [(i, k) for i in range(COUNT) for k in range(i, COUNT)]


def two_sum(a, b):
    s = a + b
    t = s - a
    return s, (a - (s - t)) + (b - t)


def split(a):
    c = a * 4097.0
    high = c - (c - a)
    return high, a - high


def pair_add(a, b):
    s, e = two_sum(a[0], b[0])
    e = e + (a[1] + b[1])
    high = s + e
    return high, e - (high - s)


def pair_mul(a, b):
    p = a[0] * b[0]
    ah, al = split(a[0])
    bh, bl = split(b[0])
    e = ((ah * bh - p) + (ah * bl + al * bh)) + al * bl
    return p, e + (a[0] * b[1] + a[1] * b[0])


def pair_times(a, b):
    p = a[0] * b
    ah, al = split(a[0])
    bh, bl = split(b)
    e = ((ah * bh - p) + (ah * bl + al * bh)) + al * bl
    return p, e + a[1] * b


def pair_neg(a):
    return -a[0], -a[1]


def pair_sum(terms):
    terms = list(terms)
    while len(terms) > 1:
        rest = terms[len(terms) // 2 * 2 :]
        terms = [pair_add(terms[i], terms[i + 1]) for i in range(0, len(terms) - 1, 2)] + rest
    return terms[0]


def over_sublanes(a):
    for shift in (4, 2, 1):
        a = pair_add(a, (pltpu.roll(a[0], shift, 0), pltpu.roll(a[1], shift, 0)))
    return a


def lanes():
    return lax.broadcasted_iota(jnp.int32, (8, 128), 1)


def as_row(a):
    return jnp.where(lanes() < 64, a[0], pltpu.roll(a[1], 64, 1))


def sum_of_rows(ref):
    blocks = [ref[pl.ds(8 * r, 8), :] for r in range(ref.shape[0] // 8)]
    return over_sublanes(pair_sum([(b, pltpu.roll(b, 64, 1)) for b in blocks]))


def edges_kernel(v_last, v_first, p_last, p_first, to_next, to_previous):
    to_next[0:8, 0:3] = p_last[:, 5:8]
    to_next[0:8, 3:8] = v_last[:, 3:8]
    to_previous[0:8, 0:5] = v_first[:, 0:5]
    to_previous[0:8, 5:8] = p_first[:, 0:3]
    for plane in range(8):
        to_next[8, plane : plane + 1] = p_last[plane, 4:5]
        to_previous[8, plane : plane + 1] = p_first[plane, 3:4]


def assemble(x, k0, dg, slot):
    def rows_of(at, n):
        return x[pl.ds(at, n), :]

    k0[slot, 5:13, 8:40] = rows_of(0, 256).reshape(8, 32, 128) * SCALE
    dg[slot, 4:12, 8:40] = rows_of(256, 256).reshape(8, 32, 128) + FIRST
    row = lax.broadcasted_iota(jnp.int32, (8, 128), 0)

    def halo(at, high, plane, fourth=None):
        tile = rows_of(at, 8)
        rows = slice(40, 48) if high else slice(0, 8)
        k0[slot, plane, rows] = tile * SCALE
        near = pltpu.roll(tile, 3 if high else 5, 0)
        if fourth is not None:
            far = jnp.broadcast_to(x[pl.ds(fourth, 1), :], (8, 128))
            near = jnp.where(row == (3 if high else 4), far, near)
        dg[slot, plane - 1, rows] = near + FIRST

    for high in (0, 1):
        start = 512 + 72 * high
        for plane in range(8):
            halo(start + 8 * plane, high, 5 + plane, start + 64 + plane)
    for side in (0, 1):
        start = 656 + 352 * side
        own, at = (13, 12) if side else (0, 0)
        k0[slot, own : own + 5, 8:40] = rows_of(start, 160).reshape(5, 32, 128) * SCALE
        dg[slot, at : at + 4, 8:40] = rows_of(start + 160, 128).reshape(4, 32, 128) + FIRST
        for high in (0, 1):
            for plane in range(4):
                halo(start + 288 + 32 * high + 8 * plane, high, (13 if side else 1) + plane)


def krylov_kernel(x, q, k_out, row_out, k0, k1, k2, k3, k4, k5, dg):
    mine = lax.axis_index("slab")
    y, z = lax.axis_index("py"), lax.axis_index("pz")
    inside = {
        "y_low": jnp.where(y > 0, 1.0, 0.0),
        "y_high": jnp.where(y < lax.axis_size("py") - 1, 1.0, 0.0),
        "z_low": jnp.where(z > 0, 1.0, 0.0),
        "z_high": jnp.where(z < lax.axis_size("pz") - 1, 1.0, 0.0),
    }
    assemble(x, k0, dg, mine)
    assemble(q, k0, dg, 1 - mine)
    lane = lax.broadcasted_iota(jnp.int32, (48, 128), 1)
    first, last = lane == 0, lane == 127
    basis = (k0, k1, k2, k3, k4, k5)
    for step in range(1, COUNT):
        old, new = basis[step - 1], basis[step]
        shift = SHIFTS[0] - SHIFTS[step - 1]
        for plane in range(step, 18 - step):
            f = [old[t, plane] for t in (0, 1)]
            up = [pltpu.roll(a, 1, 1) for a in f]
            down = [pltpu.roll(a, 127, 1) for a in f]
            beside = [
                jnp.where(first, 0.0, up[0]) + jnp.where(last, down[1], down[0]),
                jnp.where(first, up[0], up[1]) + jnp.where(last, 0.0, down[1]),
            ]
            outer = step == ITERS or plane in (step, 17 - step)
            rows = slice(8, 40) if outer else slice(0, 48)
            for t in (0, 1):
                along_y = old[t, plane, 7:39] + old[t, plane, 9:41]
                if not outer:
                    along_y = jnp.concatenate(
                        [
                            pltpu.roll(f[t][0:8], 1, 0) + old[t, plane, 1:9],
                            along_y,
                            old[t, plane, 39:47] + pltpu.roll(f[t][40:48], 7, 0),
                        ]
                    )
                around = beside[t][rows] + along_y
                around = around + (old[t, plane - 1, rows] + old[t, plane + 1, rows])
                factor = dg[t, plane - 1, rows]
                if shift != 0.0:
                    factor = factor + shift
                image = factor * f[t][rows] - around
                if step == ITERS:
                    new[t, plane - ITERS] = image
                    continue
                if plane < ITERS:
                    image = image * inside["z_low"]
                if plane >= 13:
                    image = image * inside["z_high"]
                if outer:
                    new[t, plane, rows] = image
                    continue
                new[t, plane, 0:8] = image[0:8] * inside["y_low"]
                new[t, plane, 8:40] = image[8:40]
                new[t, plane, 40:48] = image[40:48] * inside["y_high"]
    sums = [None] * len(PAIRS)
    for plane in range(8):
        for tile in range(4):
            own = [b[mine, 5 + plane, 8 + 8 * tile : 16 + 8 * tile] for b in basis[:ITERS]]
            own.append(k5[mine, plane, 8 * tile : 8 + 8 * tile])
            for i, value in enumerate(own):
                k_out[i, plane, 8 * tile : 8 + 8 * tile] = value
            parts = [split(value) for value in own]
            for n, (i, k) in enumerate(PAIRS):
                big = parts[i][0] * parts[k][0]
                small = parts[i][0] * parts[k][1] + parts[i][1] * own[k]
                if sums[n] is None:
                    sums[n] = (big, small)
                else:
                    s, e = two_sum(sums[n][0], big)
                    sums[n] = (s, sums[n][1] + (e + small))
    row = lax.broadcasted_iota(jnp.int32, (8, 128), 0)
    tables = []
    sums = [over_sublanes(s) for s in sums]
    for half in (0, 1):
        blocks = []
        for start in range(0, len(PAIRS), 8):
            block = sums[start][half]
            for n in range(start + 1, min(start + 8, len(PAIRS))):
                block = jnp.where(row == n - start, sums[n][half], block)
            blocks.append(block)
        blocks.append(jnp.zeros((128 - 8 * len(blocks), 128), jnp.float32))
        tables.append(jnp.transpose(jnp.concatenate(blocks)))
    total = over_sublanes(
        pair_sum([tuple(t[8 * r : 8 * r + 8] for t in tables) for r in range(16)])
    )
    sent = as_row(total)
    for r in range(row_out.shape[0] // 8):
        row_out[8 * r : 8 * r + 8] = sent


def rows_kernel(rows, out):
    sent = as_row(sum_of_rows(rows))
    for r in range(out.shape[0] // 8):
        out[8 * r : 8 * r + 8] = sent


def root_of(square):
    x = pair_add(square, (jnp.full_like(square[0], EPSILON), jnp.zeros_like(square[0])))
    r = lax.rsqrt(x[0])
    r = r * (1.5 - (0.5 * x[0]) * (r * r))
    one = pair_times(pair_times(x, r), r)
    miss = (1.0 - one[0]) - one[1]
    return x[0] * r, (r, r * (0.5 * miss))


def row_of(a, i):
    return tuple(jnp.broadcast_to(t[i : i + 1, :], (8, 128)) for t in a)


def pair_dot(a, b):
    return over_sublanes(pair_mul(a, b))


def coefficients(gram, ready):
    row = lax.broadcasted_iota(jnp.int32, (8, 128), 0)
    zero = jnp.zeros((8, 128), jnp.float32)
    shifts = zero
    for i, shift in enumerate(SHIFTS):
        shifts = jnp.where(row == i, shift, shifts)
    _, inverse = root_of(tuple(g * SCALE**-2 for g in row_of(gram[0], 0)))
    columns = [(jnp.where(row == 0, 1.0, zero), zero)]
    sizes = [tuple(r / SCALE for r in inverse)]
    lack = [[(EPSILON * inverse[0]) * inverse[0]]]
    alphas, betas = [], []
    for j in range(ITERS):
        newest = columns[j]
        image = pair_add(
            pair_times(newest, shifts), tuple(pltpu.roll(t, 1, 0) for t in newest)
        )
        weights = pair_sum([pair_mul(gram[k], row_of(image, k)) for k in range(j + 2)])
        dots = [pair_dot(columns[k], weights) for k in range(j + 1)]
        norm = pair_dot(image, weights)
        ready(j, columns[j], sizes[j])
        first = [pair_mul(dots[k], sizes[k]) for k in range(j + 1)]
        second = [sum(lack[k][l] * first[l][0] for l in range(j + 1)) for k in range(j + 1)]
        third = [sum(lack[k][l] * second[l] for l in range(j + 1)) for k in range(j + 1)]
        both = [pair_add(first[k], (second[k], zero)) for k in range(j + 1)]
        rest = sum(
            second[k] * second[k] - both[k][0] * (second[k] + third[k]) for k in range(j + 1)
        )
        square = pair_sum(
            [norm] + [pair_neg(pair_mul(f, f)) for f in first] + [(rest, zero)]
        )
        square = pair_mul(square, pair_mul(sizes[j], sizes[j]))
        positive = square[0] + square[1] > 0.0
        beta, inverse = root_of(tuple(jnp.where(positive, s, 0.0) for s in square))
        alphas.append(both[j][0] * sizes[j][0])
        betas.append(beta)
        columns.append(
            pair_sum(
                [image]
                + [
                    pair_neg(pair_mul(columns[k], pair_mul(both[k], sizes[k])))
                    for k in range(j + 1)
                ]
            )
        )
        sizes.append(pair_mul(sizes[j], inverse))
        for k in range(j + 1):
            lack[k].append(-third[k] * sizes[j + 1][0])
        lack.append([lack[k][j + 1] for k in range(j + 1)] + [(EPSILON * inverse[0]) * inverse[0]])
    ready(ITERS, columns[ITERS], sizes[ITERS])
    return alphas, betas


def lanczos_kernel(per_cell, rows, basis, vectors, tridiagonal, made, done):
    total = sum_of_rows(rows)
    lane, row = lanes(), lax.broadcasted_iota(jnp.int32, (8, 128), 0)
    gram = []
    for k in range(COUNT):
        low, high = jnp.minimum(row, k), jnp.maximum(row, k)
        place = low * COUNT - ((low * (low - 1)) >> 1) + (high - low)
        picked = (lane == place) & (row < COUNT)
        gram.append(
            tuple(
                jnp.broadcast_to(
                    jnp.sum(jnp.where(picked, t, 0.0), axis=1, keepdims=True) * per_cell, (8, 128)
                )
                for t in total
            )
        )

    def copy(j):
        return pltpu.make_async_copy(made.at[j], vectors.at[j], done.at[j])

    def ready(j, column, size):
        scaled = pair_mul(column, size)
        scaled = scaled[0] + scaled[1]
        factors = [jnp.broadcast_to(scaled[i : i + 1, :], (8, 128)) for i in range(j + 1)]
        for plane in range(8):
            for tile in range(4):
                at = slice(8 * tile, 8 * tile + 8)
                value = factors[0] * basis[0, plane, at]
                for i in range(1, j + 1):
                    value = value + factors[i] * basis[i, plane, at]
                made[j, plane, at] = value
        copy(j).start()

    alphas, betas = coefficients(gram, ready)
    for r, values in enumerate((alphas, betas)):
        table = jnp.zeros((8, 128), jnp.float32)
        for j, value in enumerate(values):
            table = jnp.where(lane == j, value, table)
        tridiagonal[r : r + 1, :] = table[0:1, 0:ITERS]
    for j in range(COUNT):
        copy(j).wait()


def call(kernel, out_shape, scratch=(), flops=10000, mebibytes=4, **specs):
    return pl.pallas_call(
        kernel,
        out_shape=out_shape,
        scratch_shapes=list(scratch),
        cost_estimate=pl.CostEstimate(flops=flops, bytes_accessed=flops, transcendentals=0),
        compiler_params=pltpu.CompilerParams(
            vmem_limit_bytes=mebibytes and mebibytes * 2**20
        ),
        interpret=INTERPRET,
        **specs,
    )


def to_rows(*pieces):
    return jnp.concatenate([p.reshape(-1, 128) for p in pieces])


def shards(v, p):
    f32 = jnp.float32

    def line(axis, step):
        n = lax.axis_size(axis)
        return [(i, i + step) for i in range(n) if 0 <= i + step < n]

    def exchange(to_next, to_previous, axis):
        return (
            lax.ppermute(to_next, axis, line(axis, 1)),
            lax.ppermute(to_previous, axis, line(axis, -1)),
        )

    halo = jax.ShapeDtypeStruct((9, 8, 128), f32)
    last, first = slice(24, 32), slice(0, 8)
    y_low, y_high = exchange(
        *call(edges_kernel, (halo, halo), mebibytes=1)(
            v[:, last], v[:, first], p[:, last], p[:, first]
        ),
        "py",
    )
    z_low, z_high = exchange(
        to_rows(v[3:], p[4:], y_low[4:8], y_high[4:8]),
        to_rows(v[:5], p[:4], y_low[:4], y_high[:4]),
        "pz",
    )
    x = to_rows(v, p, y_low, y_high, z_low, z_high)
    q = lax.ppermute(x, "slab", [(0, 1), (1, 0)])
    n_z = lax.axis_size("pz")
    n_xy = lax.axis_size("slab") * lax.axis_size("py")
    block = [pltpu.VMEM((2, 18, 48, 128), f32)] * 5
    basis, rows = call(
        krylov_kernel,
        (jax.ShapeDtypeStruct((COUNT, 8, 32, 128), f32), jax.ShapeDtypeStruct((n_z, 128), f32)),
        block + [pltpu.VMEM((2, 8, 32, 128), f32), pltpu.VMEM((2, 16, 48, 128), f32)],
        20000000,
        12,
    )(x, q)
    rows = lax.all_to_all(rows, "pz", 0, 0, tiled=True)
    rows = call(rows_kernel, jax.ShapeDtypeStruct((n_xy, 128), f32))(rows)
    rows = lax.all_to_all(rows, ("slab", "py"), 0, 0, tiled=True)
    per_cell = 1.0 / (v.size * n_z * n_xy)
    return call(
        functools.partial(lanczos_kernel, per_cell),
        (
            jax.ShapeDtypeStruct((COUNT, 8, 32, 128), f32),
            jax.ShapeDtypeStruct((2, ITERS), f32),
        ),
        [pltpu.VMEM((COUNT, 8, 32, 128), f32), pltpu.SemaphoreType.DMA((COUNT,))],
        flops=20000000,
        out_specs=(
            pl.BlockSpec(memory_space=pl.ANY),
            pl.BlockSpec(memory_space=pltpu.VMEM),
        ),
    )(rows, basis)


def solution(mesh):
    in_specs = (P("pz", "py", "slab"), P("pz", "py", "slab"))
    out_specs = (P(None, "pz", "py", "slab"), P())
    return jax.shard_map(shards, mesh=mesh, in_specs=in_specs, out_specs=out_specs, check_vma=False)
```

```python
import functools

import jax
import jax.numpy as jnp
from jax import lax
from jax.experimental import pallas as pl
from jax.experimental.pallas import tpu as pltpu
from jax.sharding import PartitionSpec as P

ITERS = 5
EPSILON = 1e-06
INTERPRET = False

SHIFTS = (2.25, 14.25, 8.25, 2.25, 14.25)
SCALE = 2.0**24
FIRST = 6.0 - SHIFTS[0]
COUNT = ITERS + 1
PAIRS = [(i, k) for i in range(COUNT) for k in range(i, COUNT)]


def two_sum(a, b):
    s = a + b
    t = s - a
    return s, (a - (s - t)) + (b - t)


def split(a):
    c = a * 4097.0
    high = c - (c - a)
    return high, a - high


def pair_add(a, b):
    s, e = two_sum(a[0], b[0])
    e = e + (a[1] + b[1])
    high = s + e
    return high, e - (high - s)


def pair_mul(a, b):
    p = a[0] * b[0]
    ah, al = split(a[0])
    bh, bl = split(b[0])
    e = ((ah * bh - p) + (ah * bl + al * bh)) + al * bl
    return p, e + (a[0] * b[1] + a[1] * b[0])


def pair_times(a, b):
    p = a[0] * b
    ah, al = split(a[0])
    bh, bl = split(b)
    e = ((ah * bh - p) + (ah * bl + al * bh)) + al * bl
    return p, e + a[1] * b


def pair_neg(a):
    return -a[0], -a[1]


def pair_sum(terms):
    terms = list(terms)
    while len(terms) > 1:
        rest = terms[len(terms) // 2 * 2 :]
        terms = [pair_add(terms[i], terms[i + 1]) for i in range(0, len(terms) - 1, 2)] + rest
    return terms[0]


def over_sublanes(a):
    for shift in (4, 2, 1):
        a = pair_add(a, (pltpu.roll(a[0], shift, 0), pltpu.roll(a[1], shift, 0)))
    return a


def lanes():
    return lax.broadcasted_iota(jnp.int32, (8, 128), 1)


def as_row(a):
    return jnp.where(lanes() < 64, a[0], pltpu.roll(a[1], 64, 1))


def sum_of_rows(ref):
    blocks = [ref[pl.ds(8 * r, 8), :] for r in range(ref.shape[0] // 8)]
    return over_sublanes(pair_sum([(b, pltpu.roll(b, 64, 1)) for b in blocks]))


def edges_kernel(v_last, v_first, p_last, p_first, to_next, to_previous):
    to_next[0:8, 0:3] = p_last[:, 5:8]
    to_next[0:8, 3:8] = v_last[:, 3:8]
    to_previous[0:8, 0:5] = v_first[:, 0:5]
    to_previous[0:8, 5:8] = p_first[:, 0:3]
    for plane in range(8):
        to_next[8, plane : plane + 1] = p_last[plane, 4:5]
        to_previous[8, plane : plane + 1] = p_first[plane, 3:4]


def blocks_of(refs):
    v, p, y_low, y_high, z_low, z_high = refs
    tiles = [(ref, (plane, pl.ds(8 * r, 8))) for ref in (v, p) for plane in range(8) for r in range(4)]
    tiles += [(ref, (plane, pl.ds(0, 8))) for ref in (y_low, y_high) for plane in range(9)]
    return tiles + [(ref, (pl.ds(8 * r, 8),)) for ref in (z_low, z_high) for r in range(44)]


def side_kernel(*refs):
    out = refs[-1]
    mine = lax.axis_index("slab")
    lane = lanes()
    tiles = blocks_of(refs[:-1])
    for start in range(0, len(tiles), 16):
        packed = jnp.zeros((8, 128), jnp.float32)
        for k, (ref, at) in enumerate(tiles[start : start + 16]):
            moved = pltpu.roll(ref[at], lax.rem(8 * k + 8 * (1 - mine), 128), 1)
            packed = jnp.where((lane >= 8 * k) & (lane < 8 * k + 8), moved, packed)
        out[start // 2 : start // 2 + 8] = packed


def assemble(tile_of, k0, dg, slot):
    row = lax.broadcasted_iota(jnp.int32, (8, 128), 0)

    def halo(tile, high, plane, fourth=None):
        rows = slice(40, 48) if high else slice(0, 8)
        k0[slot, plane, rows] = tile * SCALE
        near = pltpu.roll(tile, 3 if high else 5, 0)
        if fourth is not None:
            near = jnp.where(row == (3 if high else 4), jnp.broadcast_to(fourth, (8, 128)), near)
        dg[slot, plane - 1, rows] = near + FIRST

    def inner(ref, plane, r, value):
        ref[slot, plane, 8 + 8 * r : 16 + 8 * r] = value

    for plane in range(8):
        for r in range(4):
            inner(k0, 5 + plane, r, tile_of(4 * plane + r) * SCALE)
            inner(dg, 4 + plane, r, tile_of(32 + 4 * plane + r) + FIRST)
    for high in (0, 1):
        start = 64 + 9 * high
        fourths = tile_of(start + 8)
        for plane in range(8):
            halo(tile_of(start + plane), high, 5 + plane, fourths[plane : plane + 1])
    for side in (0, 1):
        start = 82 + 44 * side
        for plane in range(5):
            for r in range(4):
                inner(k0, (13 if side else 0) + plane, r, tile_of(start + 4 * plane + r) * SCALE)
        for plane in range(4):
            for r in range(4):
                value = tile_of(start + 20 + 4 * plane + r) + FIRST
                inner(dg, (12 if side else 0) + plane, r, value)
        for high in (0, 1):
            for plane in range(4):
                tile = tile_of(start + 36 + 4 * high + plane)
                halo(tile, high, (13 if side else 1) + plane)


def krylov_kernel(v, p, y_low, y_high, z_low, z_high, side, k_out, row_out, k0, k1, k2, k3, k4, k5, dg):
    mine = lax.axis_index("slab")
    y, z = lax.axis_index("py"), lax.axis_index("pz")
    inside = {
        "y_low": jnp.where(y > 0, 1.0, 0.0),
        "y_high": jnp.where(y < lax.axis_size("py") - 1, 1.0, 0.0),
        "z_low": jnp.where(z > 0, 1.0, 0.0),
        "z_high": jnp.where(z < lax.axis_size("pz") - 1, 1.0, 0.0),
    }
    lane = lax.broadcasted_iota(jnp.int32, (48, 128), 1)
    first, last = lane == 0, lane == 127
    near = (lane >= 120 * mine) & (lane < 8 + 120 * mine)
    near8 = near[0:8]
    tiles = blocks_of((v, p, y_low, y_high, z_low, z_high))

    def own_tile(n):
        ref, at = tiles[n]
        return ref[at]

    def other_tile(n):
        k = n % 16
        shift = lax.rem(120 * mine + 128 - 8 * k, 128)
        return jnp.where(near8, pltpu.roll(side[pl.ds(n // 16 * 8, 8), :], shift, 1), 0.0)

    assemble(own_tile, k0, dg, 0)
    assemble(other_tile, k0, dg, 1)
    basis = (k0, k1, k2, k3, k4, k5)
    for step in range(1, COUNT):
        old, new = basis[step - 1], basis[step]
        shift = SHIFTS[0] - SHIFTS[step - 1]
        for plane in range(step, 18 - step):
            away = max(5 - plane, plane - 12, 0)
            f = [old[t, plane] for t in (0, 1)]
            up = [pltpu.roll(a, 1, 1) for a in f]
            down = [pltpu.roll(a, 127, 1) for a in f]
            for t in (0, 1):
                reach = ITERS - step - t - away
                if reach < 0:
                    continue
                beside = jnp.where(first, up[1 - t], up[t]) + jnp.where(last, down[1 - t], down[t])
                rows = slice(0, 48) if reach > 0 else slice(8, 40)
                along_y = old[t, plane, 7:39] + old[t, plane, 9:41]
                if reach > 0:
                    along_y = jnp.concatenate(
                        [
                            pltpu.roll(f[t][0:8], 1, 0) + old[t, plane, 1:9],
                            along_y,
                            old[t, plane, 39:47] + pltpu.roll(f[t][40:48], 7, 0),
                        ]
                    )
                around = beside[rows] + along_y
                around = around + (old[t, plane - 1, rows] + old[t, plane + 1, rows])
                factor = dg[t, plane - 1, rows]
                if shift != 0.0:
                    factor = factor + shift
                image = factor * f[t][rows] - around
                if t == 1:
                    image = jnp.where(near[rows], image, 0.0)
                if step == ITERS:
                    new[plane - ITERS] = image
                    continue
                if plane < ITERS:
                    image = image * inside["z_low"]
                if plane >= 13:
                    image = image * inside["z_high"]
                if reach == 0:
                    new[t, plane, rows] = image
                    continue
                new[t, plane, 0:8] = image[0:8] * inside["y_low"]
                new[t, plane, 8:40] = image[8:40]
                new[t, plane, 40:48] = image[40:48] * inside["y_high"]
    sums = [None] * len(PAIRS)
    for plane in range(8):
        for tile in range(4):
            own = [b[0, 5 + plane, 8 + 8 * tile : 16 + 8 * tile] for b in basis[:ITERS]]
            own.append(k5[plane, 8 * tile : 8 + 8 * tile])
            for i, value in enumerate(own):
                k_out[i, plane, 8 * tile : 8 + 8 * tile] = value
            parts = [split(value) for value in own]
            for n, (i, k) in enumerate(PAIRS):
                big = parts[i][0] * parts[k][0]
                small = parts[i][0] * parts[k][1] + parts[i][1] * own[k]
                if sums[n] is None:
                    sums[n] = (big, small)
                else:
                    s, e = two_sum(sums[n][0], big)
                    sums[n] = (s, sums[n][1] + (e + small))
    row = lax.broadcasted_iota(jnp.int32, (8, 128), 0)
    tables = []
    sums = [over_sublanes(s) for s in sums]
    for half in (0, 1):
        blocks = []
        for start in range(0, len(PAIRS), 8):
            block = sums[start][half]
            for n in range(start + 1, min(start + 8, len(PAIRS))):
                block = jnp.where(row == n - start, sums[n][half], block)
            blocks.append(block)
        blocks.append(jnp.zeros((128 - 8 * len(blocks), 128), jnp.float32))
        tables.append(jnp.transpose(jnp.concatenate(blocks)))
    total = over_sublanes(
        pair_sum([tuple(t[8 * r : 8 * r + 8] for t in tables) for r in range(16)])
    )
    sent = as_row(total)
    for r in range(row_out.shape[0] // 8):
        row_out[8 * r : 8 * r + 8] = sent


def rows_kernel(rows, out):
    sent = as_row(sum_of_rows(rows))
    for r in range(out.shape[0] // 8):
        out[8 * r : 8 * r + 8] = sent


def root_of(square):
    x = pair_add(square, (jnp.full_like(square[0], EPSILON), jnp.zeros_like(square[0])))
    r = lax.rsqrt(x[0])
    r = r * (1.5 - (0.5 * x[0]) * (r * r))
    one = pair_times(pair_times(x, r), r)
    miss = (1.0 - one[0]) - one[1]
    return x[0] * r, (r, r * (0.5 * miss))


def row_of(a, i):
    return tuple(jnp.broadcast_to(t[i : i + 1, :], (8, 128)) for t in a)


def pair_dot(a, b):
    return over_sublanes(pair_mul(a, b))


def coefficients(gram, ready):
    row = lax.broadcasted_iota(jnp.int32, (8, 128), 0)
    zero = jnp.zeros((8, 128), jnp.float32)
    shifts = zero
    for i, shift in enumerate(SHIFTS):
        shifts = jnp.where(row == i, shift, shifts)
    _, inverse = root_of(tuple(g * SCALE**-2 for g in row_of(gram[0], 0)))
    columns = [(jnp.where(row == 0, 1.0, zero), zero)]
    sizes = [tuple(r / SCALE for r in inverse)]
    lack = [[(EPSILON * inverse[0]) * inverse[0]]]
    alphas, betas = [], []
    for j in range(ITERS):
        newest = columns[j]
        image = pair_add(
            pair_times(newest, shifts), tuple(pltpu.roll(t, 1, 0) for t in newest)
        )
        weights = pair_sum([pair_mul(gram[k], row_of(image, k)) for k in range(j + 2)])
        dots = [pair_dot(columns[k], weights) for k in range(j + 1)]
        norm = pair_dot(image, weights)
        ready(j, columns[j], sizes[j])
        first = [pair_mul(dots[k], sizes[k]) for k in range(j + 1)]
        second = [sum(lack[k][l] * first[l][0] for l in range(j + 1)) for k in range(j + 1)]
        third = [sum(lack[k][l] * second[l] for l in range(j + 1)) for k in range(j + 1)]
        both = [pair_add(first[k], (second[k], zero)) for k in range(j + 1)]
        rest = sum(
            second[k] * second[k] - both[k][0] * (second[k] + third[k]) for k in range(j + 1)
        )
        square = pair_sum(
            [norm] + [pair_neg(pair_mul(f, f)) for f in first] + [(rest, zero)]
        )
        square = pair_mul(square, pair_mul(sizes[j], sizes[j]))
        positive = square[0] + square[1] > 0.0
        beta, inverse = root_of(tuple(jnp.where(positive, s, 0.0) for s in square))
        alphas.append(both[j][0] * sizes[j][0])
        betas.append(beta)
        columns.append(
            pair_sum(
                [image]
                + [
                    pair_neg(pair_mul(columns[k], pair_mul(both[k], sizes[k])))
                    for k in range(j + 1)
                ]
            )
        )
        sizes.append(pair_mul(sizes[j], inverse))
        for k in range(j + 1):
            lack[k].append(-third[k] * sizes[j + 1][0])
        lack.append([lack[k][j + 1] for k in range(j + 1)] + [(EPSILON * inverse[0]) * inverse[0]])
    ready(ITERS, columns[ITERS], sizes[ITERS])
    return alphas, betas


def lanczos_kernel(per_cell, rows, basis, vectors, tridiagonal, made, small, done):
    total = sum_of_rows(rows)
    lane, row = lanes(), lax.broadcasted_iota(jnp.int32, (8, 128), 0)
    gram = []
    for k in range(COUNT):
        low, high = jnp.minimum(row, k), jnp.maximum(row, k)
        place = low * COUNT - ((low * (low - 1)) >> 1) + (high - low)
        picked = (lane == place) & (row < COUNT)
        gram.append(
            tuple(
                jnp.broadcast_to(
                    jnp.sum(jnp.where(picked, t, 0.0), axis=1, keepdims=True) * per_cell, (8, 128)
                )
                for t in total
            )
        )

    def copy(j):
        return pltpu.make_async_copy(made.at[j], vectors.at[j], done.at[j])

    def ready(j, column, size):
        scaled = pair_mul(column, size)
        scaled = scaled[0] + scaled[1]
        factors = [jnp.broadcast_to(scaled[i : i + 1, :], (8, 128)) for i in range(j + 1)]
        for plane in range(8):
            for tile in range(4):
                at = slice(8 * tile, 8 * tile + 8)
                value = factors[0] * basis[0, plane, at]
                for i in range(1, j + 1):
                    value = value + factors[i] * basis[i, plane, at]
                made[j, plane, at] = value
        copy(j).start()

    alphas, betas = coefficients(gram, ready)
    for r, values in enumerate((alphas, betas)):
        table = jnp.zeros((8, 128), jnp.float32)
        for j, value in enumerate(values):
            table = jnp.where(lane == j, value, table)
        small[r : r + 1, :] = table[0:1, 0:ITERS]
    last = pltpu.make_async_copy(small, tridiagonal, done.at[COUNT])
    last.start()
    for j in range(COUNT):
        copy(j).wait()
    last.wait()


def call(kernel, out_shape, scratch=(), flops=10000, mebibytes=4, **specs):
    return pl.pallas_call(
        kernel,
        out_shape=out_shape,
        scratch_shapes=list(scratch),
        cost_estimate=pl.CostEstimate(flops=flops, bytes_accessed=flops, transcendentals=0),
        compiler_params=pltpu.CompilerParams(
            vmem_limit_bytes=mebibytes and mebibytes * 2**20
        ),
        interpret=INTERPRET,
        **specs,
    )


def to_rows(*pieces):
    return jnp.concatenate([p.reshape(-1, 128) for p in pieces])


def shards(v, p):
    f32 = jnp.float32

    def line(axis, step):
        n = lax.axis_size(axis)
        return [(i, i + step) for i in range(n) if 0 <= i + step < n]

    def exchange(to_next, to_previous, axis):
        return (
            lax.ppermute(to_next, axis, line(axis, 1)),
            lax.ppermute(to_previous, axis, line(axis, -1)),
        )

    halo = jax.ShapeDtypeStruct((9, 8, 128), f32)
    last, first = slice(24, 32), slice(0, 8)
    y_low, y_high = exchange(
        *call(edges_kernel, (halo, halo), mebibytes=1)(
            v[:, last], v[:, first], p[:, last], p[:, first]
        ),
        "py",
    )
    z_low, z_high = exchange(
        to_rows(v[3:], p[4:], y_low[4:8], y_high[4:8]),
        to_rows(v[:5], p[:4], y_low[:4], y_high[:4]),
        "pz",
    )
    blocks = (v, p, y_low, y_high, z_low, z_high)
    side = call(side_kernel, jax.ShapeDtypeStruct((88, 128), f32))(*blocks)
    side = lax.ppermute(side, "slab", [(0, 1), (1, 0)])
    n_z = lax.axis_size("pz")
    n_xy = lax.axis_size("slab") * lax.axis_size("py")
    block = [pltpu.VMEM((2, 18, 48, 128), f32)] * 5
    basis, rows = call(
        krylov_kernel,
        (jax.ShapeDtypeStruct((COUNT, 8, 32, 128), f32), jax.ShapeDtypeStruct((n_z, 128), f32)),
        block + [pltpu.VMEM((8, 32, 128), f32), pltpu.VMEM((2, 16, 48, 128), f32)],
        20000000,
        12,
    )(*blocks, side)
    rows = lax.all_to_all(rows, "pz", 0, 0, tiled=True)
    rows = call(rows_kernel, jax.ShapeDtypeStruct((n_xy, 128), f32))(rows)
    rows = lax.all_to_all(rows, ("slab", "py"), 0, 0, tiled=True)
    per_cell = 1.0 / (v.size * n_z * n_xy)
    return call(
        functools.partial(lanczos_kernel, per_cell),
        (
            jax.ShapeDtypeStruct((COUNT, 8, 32, 128), f32),
            jax.ShapeDtypeStruct((2, ITERS), f32),
        ),
        [
            pltpu.VMEM((COUNT, 8, 32, 128), f32),
            pltpu.VMEM((2, ITERS), f32),
            pltpu.SemaphoreType.DMA((COUNT + 1,)),
        ],
        flops=20000000,
        out_specs=(pl.BlockSpec(memory_space=pl.ANY),) * 2,
    )(rows, basis)


def solution(mesh):
    in_specs = (P("pz", "py", "slab"), P("pz", "py", "slab"))
    out_specs = (P(None, "pz", "py", "slab"), P())
    return jax.shard_map(shards, mesh=mesh, in_specs=in_specs, out_specs=out_specs, check_vma=False)
```

```python
import functools

import jax
import jax.numpy as jnp
from jax import lax
from jax.experimental import pallas as pl
from jax.experimental.pallas import tpu as pltpu
from jax.sharding import PartitionSpec as P

ITERS = 5
EPSILON = 1e-06
INTERPRET = False

SHIFTS = (1.25, 3.25, 8.25, 14.25, 4.25)
SCALE = 2.0**24
FIRST = 6.0 - SHIFTS[0]
COUNT = ITERS + 1
PAIRS = [(i, k) for i in range(COUNT) for k in range(i, COUNT)]


def two_sum(a, b):
    s = a + b
    t = s - a
    return s, (a - (s - t)) + (b - t)


def split(a):
    c = a * 4097.0
    high = c - (c - a)
    return high, a - high


def pair_add(a, b):
    s, e = two_sum(a[0], b[0])
    e = e + (a[1] + b[1])
    high = s + e
    return high, e - (high - s)


def pair_mul(a, b):
    p = a[0] * b[0]
    ah, al = split(a[0])
    bh, bl = split(b[0])
    e = ((ah * bh - p) + (ah * bl + al * bh)) + al * bl
    return p, e + (a[0] * b[1] + a[1] * b[0])


def pair_times(a, b):
    p = a[0] * b
    ah, al = split(a[0])
    bh, bl = split(b)
    e = ((ah * bh - p) + (ah * bl + al * bh)) + al * bl
    return p, e + a[1] * b


def pair_neg(a):
    return -a[0], -a[1]


def pair_sum(terms):
    terms = list(terms)
    while len(terms) > 1:
        rest = terms[len(terms) // 2 * 2 :]
        terms = [pair_add(terms[i], terms[i + 1]) for i in range(0, len(terms) - 1, 2)] + rest
    return terms[0]


def over_sublanes(a):
    for shift in (4, 2, 1):
        a = pair_add(a, (pltpu.roll(a[0], shift, 0), pltpu.roll(a[1], shift, 0)))
    return a


def lanes():
    return lax.broadcasted_iota(jnp.int32, (8, 128), 1)


def as_row(a):
    return jnp.where(lanes() < 64, a[0], pltpu.roll(a[1], 64, 1))


def sum_of_rows(ref):
    blocks = [ref[pl.ds(8 * r, 8), :] for r in range(ref.shape[0] // 8)]
    return over_sublanes(pair_sum([(b, pltpu.roll(b, 64, 1)) for b in blocks]))


def edges_kernel(v_last, v_first, p_last, p_first, to_next, to_previous):
    to_next[0:8, 0:3] = p_last[:, 5:8]
    to_next[0:8, 3:8] = v_last[:, 3:8]
    to_previous[0:8, 0:5] = v_first[:, 0:5]
    to_previous[0:8, 5:8] = p_first[:, 0:3]
    for plane in range(8):
        to_next[8, plane : plane + 1] = p_last[plane, 4:5]
        to_previous[8, plane : plane + 1] = p_first[plane, 3:4]


def blocks_of(refs):
    v, p, y_low, y_high, z_low, z_high = refs
    tiles = [(ref, (plane, pl.ds(8 * r, 8))) for ref in (v, p) for plane in range(8) for r in range(4)]
    tiles += [(ref, (plane, pl.ds(0, 8))) for ref in (y_low, y_high) for plane in range(9)]
    return tiles + [(ref, (pl.ds(8 * r, 8),)) for ref in (z_low, z_high) for r in range(44)]


def side_kernel(*refs):
    out = refs[-1]
    mine = lax.axis_index("slab")
    lane = lanes()
    tiles = blocks_of(refs[:-1])
    for start in range(0, len(tiles), 16):
        packed = jnp.zeros((8, 128), jnp.float32)
        for k, (ref, at) in enumerate(tiles[start : start + 16]):
            moved = pltpu.roll(ref[at], lax.rem(8 * k + 8 * (1 - mine), 128), 1)
            packed = jnp.where((lane >= 8 * k) & (lane < 8 * k + 8), moved, packed)
        out[start // 2 : start // 2 + 8] = packed


def assemble(tile_of, k0, dg, slot):
    row = lax.broadcasted_iota(jnp.int32, (8, 128), 0)

    def halo(tile, high, plane, fourth=None):
        rows = slice(40, 48) if high else slice(0, 8)
        k0[slot, plane, rows] = tile * SCALE
        near = pltpu.roll(tile, 3 if high else 5, 0)
        if fourth is not None:
            near = jnp.where(row == (3 if high else 4), jnp.broadcast_to(fourth, (8, 128)), near)
        dg[slot, plane - 1, rows] = near + FIRST

    def inner(ref, plane, r, value):
        ref[slot, plane, 8 + 8 * r : 16 + 8 * r] = value

    for plane in range(8):
        for r in range(4):
            inner(k0, 5 + plane, r, tile_of(4 * plane + r) * SCALE)
            inner(dg, 4 + plane, r, tile_of(32 + 4 * plane + r) + FIRST)
    for high in (0, 1):
        start = 64 + 9 * high
        fourths = tile_of(start + 8)
        for plane in range(8):
            halo(tile_of(start + plane), high, 5 + plane, fourths[plane : plane + 1])
    for side in (0, 1):
        start = 82 + 44 * side
        for plane in range(5):
            for r in range(4):
                inner(k0, (13 if side else 0) + plane, r, tile_of(start + 4 * plane + r) * SCALE)
        for plane in range(4):
            for r in range(4):
                value = tile_of(start + 20 + 4 * plane + r) + FIRST
                inner(dg, (12 if side else 0) + plane, r, value)
        for high in (0, 1):
            for plane in range(4):
                tile = tile_of(start + 36 + 4 * high + plane)
                halo(tile, high, (13 if side else 1) + plane)


def krylov_kernel(v, p, y_low, y_high, z_low, z_high, side, k_out, row_out, k0, k1, k2, k3, k4, k5, dg):
    mine = lax.axis_index("slab")
    y, z = lax.axis_index("py"), lax.axis_index("pz")
    inside = {
        "y_low": jnp.where(y > 0, 1.0, 0.0),
        "y_high": jnp.where(y < lax.axis_size("py") - 1, 1.0, 0.0),
        "z_low": jnp.where(z > 0, 1.0, 0.0),
        "z_high": jnp.where(z < lax.axis_size("pz") - 1, 1.0, 0.0),
    }
    lane = lax.broadcasted_iota(jnp.int32, (48, 128), 1)
    first, last = lane == 0, lane == 127
    near = (lane >= 120 * mine) & (lane < 8 + 120 * mine)
    near8 = near[0:8]
    tiles = blocks_of((v, p, y_low, y_high, z_low, z_high))

    def own_tile(n):
        ref, at = tiles[n]
        return ref[at]

    def other_tile(n):
        k = n % 16
        shift = lax.rem(120 * mine + 128 - 8 * k, 128)
        return jnp.where(near8, pltpu.roll(side[pl.ds(n // 16 * 8, 8), :], shift, 1), 0.0)

    assemble(own_tile, k0, dg, 0)
    assemble(other_tile, k0, dg, 1)
    basis = (k0, k1, k2, k3, k4, k5)
    for step in range(1, COUNT):
        old, new = basis[step - 1], basis[step]
        shift = SHIFTS[0] - SHIFTS[step - 1]
        for plane in range(step, 18 - step):
            away = max(5 - plane, plane - 12, 0)
            f = [old[t, plane] for t in (0, 1)]
            up = [pltpu.roll(a, 1, 1) for a in f]
            down = [pltpu.roll(a, 127, 1) for a in f]
            for t in (0, 1):
                reach = ITERS - step - t - away
                if reach < 0:
                    continue
                beside = jnp.where(first, up[1 - t], up[t]) + jnp.where(last, down[1 - t], down[t])
                rows = slice(0, 48) if reach > 0 else slice(8, 40)
                along_y = old[t, plane, 7:39] + old[t, plane, 9:41]
                if reach > 0:
                    along_y = jnp.concatenate(
                        [
                            pltpu.roll(f[t][0:8], 1, 0) + old[t, plane, 1:9],
                            along_y,
                            old[t, plane, 39:47] + pltpu.roll(f[t][40:48], 7, 0),
                        ]
                    )
                around = beside[rows] + along_y
                around = around + (old[t, plane - 1, rows] + old[t, plane + 1, rows])
                factor = dg[t, plane - 1, rows]
                if shift != 0.0:
                    factor = factor + shift
                image = factor * f[t][rows] - around
                if t == 1:
                    image = jnp.where(near[rows], image, 0.0)
                if step == ITERS:
                    new[plane - ITERS] = image
                    continue
                if plane < ITERS:
                    image = image * inside["z_low"]
                if plane >= 13:
                    image = image * inside["z_high"]
                if reach == 0:
                    new[t, plane, rows] = image
                    continue
                new[t, plane, 0:8] = image[0:8] * inside["y_low"]
                new[t, plane, 8:40] = image[8:40]
                new[t, plane, 40:48] = image[40:48] * inside["y_high"]
    sums = [None] * len(PAIRS)
    for plane in range(8):
        for tile in range(4):
            own = [b[0, 5 + plane, 8 + 8 * tile : 16 + 8 * tile] for b in basis[:ITERS]]
            own.append(k5[plane, 8 * tile : 8 + 8 * tile])
            for i, value in enumerate(own):
                k_out[i, plane, 8 * tile : 8 + 8 * tile] = value
            parts = [split(value) for value in own]
            for n, (i, k) in enumerate(PAIRS):
                big = parts[i][0] * parts[k][0]
                small = parts[i][0] * parts[k][1] + parts[i][1] * own[k]
                if sums[n] is None:
                    sums[n] = (big, small)
                else:
                    s, e = two_sum(sums[n][0], big)
                    sums[n] = (s, sums[n][1] + (e + small))
    row = lax.broadcasted_iota(jnp.int32, (8, 128), 0)
    tables = []
    sums = [over_sublanes(s) for s in sums]
    for half in (0, 1):
        blocks = []
        for start in range(0, len(PAIRS), 8):
            block = sums[start][half]
            for n in range(start + 1, min(start + 8, len(PAIRS))):
                block = jnp.where(row == n - start, sums[n][half], block)
            blocks.append(block)
        blocks.append(jnp.zeros((128 - 8 * len(blocks), 128), jnp.float32))
        tables.append(jnp.transpose(jnp.concatenate(blocks)))
    total = over_sublanes(
        pair_sum([tuple(t[8 * r : 8 * r + 8] for t in tables) for r in range(16)])
    )
    sent = as_row(total)
    for r in range(row_out.shape[0] // 8):
        row_out[8 * r : 8 * r + 8] = sent


def rows_kernel(rows, out):
    sent = as_row(sum_of_rows(rows))
    for r in range(out.shape[0] // 8):
        out[8 * r : 8 * r + 8] = sent


def root_of(square):
    x = pair_add(square, (jnp.full_like(square[0], EPSILON), jnp.zeros_like(square[0])))
    r = lax.rsqrt(x[0])
    r = r * (1.5 - (0.5 * x[0]) * (r * r))
    one = pair_times(pair_times(x, r), r)
    miss = (1.0 - one[0]) - one[1]
    return x[0] * r, (r, r * (0.5 * miss))


def row_of(a, i):
    return tuple(jnp.broadcast_to(t[i : i + 1, :], (8, 128)) for t in a)


def pair_dot(a, b):
    return over_sublanes(pair_mul(a, b))


def coefficients(gram, ready):
    row = lax.broadcasted_iota(jnp.int32, (8, 128), 0)
    zero = jnp.zeros((8, 128), jnp.float32)
    shifts = zero
    for i, shift in enumerate(SHIFTS):
        shifts = jnp.where(row == i, shift, shifts)
    _, inverse = root_of(tuple(g * SCALE**-2 for g in row_of(gram[0], 0)))
    columns = [(jnp.where(row == 0, 1.0, zero), zero)]
    sizes = [tuple(r / SCALE for r in inverse)]
    lack = [[(EPSILON * inverse[0]) * inverse[0]]]
    alphas, betas = [], []
    for j in range(ITERS):
        newest = columns[j]
        image = pair_add(
            pair_times(newest, shifts), tuple(pltpu.roll(t, 1, 0) for t in newest)
        )
        weights = pair_sum([pair_mul(gram[k], row_of(image, k)) for k in range(j + 2)])
        dots = [pair_dot(columns[k], weights) for k in range(j + 1)]
        norm = pair_dot(image, weights)
        ready(j, columns[j], sizes[j])
        first = [pair_mul(dots[k], sizes[k]) for k in range(j + 1)]
        second = [sum(lack[k][l] * first[l][0] for l in range(j + 1)) for k in range(j + 1)]
        third = [sum(lack[k][l] * second[l] for l in range(j + 1)) for k in range(j + 1)]
        both = [pair_add(first[k], (second[k], zero)) for k in range(j + 1)]
        rest = sum(
            second[k] * second[k] - both[k][0] * (second[k] + third[k]) for k in range(j + 1)
        )
        square = pair_sum(
            [norm] + [pair_neg(pair_mul(f, f)) for f in first] + [(rest, zero)]
        )
        square = pair_mul(square, pair_mul(sizes[j], sizes[j]))
        positive = square[0] + square[1] > 0.0
        beta, inverse = root_of(tuple(jnp.where(positive, s, 0.0) for s in square))
        alphas.append(both[j][0] * sizes[j][0])
        betas.append(beta)
        columns.append(
            pair_sum(
                [image]
                + [
                    pair_neg(pair_mul(columns[k], pair_mul(both[k], sizes[k])))
                    for k in range(j + 1)
                ]
            )
        )
        sizes.append(pair_mul(sizes[j], inverse))
        for k in range(j + 1):
            lack[k].append(-third[k] * sizes[j + 1][0])
        lack.append([lack[k][j + 1] for k in range(j + 1)] + [(EPSILON * inverse[0]) * inverse[0]])
    ready(ITERS, columns[ITERS], sizes[ITERS])
    return alphas, betas


def lanczos_kernel(per_cell, rows, basis, vectors, tridiagonal, made, small, done):
    total = sum_of_rows(rows)
    lane, row = lanes(), lax.broadcasted_iota(jnp.int32, (8, 128), 0)
    gram = []
    for k in range(COUNT):
        low, high = jnp.minimum(row, k), jnp.maximum(row, k)
        place = low * COUNT - ((low * (low - 1)) >> 1) + (high - low)
        picked = (lane == place) & (row < COUNT)
        gram.append(
            tuple(
                jnp.broadcast_to(
                    jnp.sum(jnp.where(picked, t, 0.0), axis=1, keepdims=True) * per_cell, (8, 128)
                )
                for t in total
            )
        )

    def copy(j):
        return pltpu.make_async_copy(made.at[j], vectors.at[j], done.at[j])

    def ready(j, column, size):
        scaled = pair_mul(column, size)
        scaled = scaled[0] + scaled[1]
        factors = [jnp.broadcast_to(scaled[i : i + 1, :], (8, 128)) for i in range(j + 1)]
        for plane in range(8):
            for tile in range(4):
                at = slice(8 * tile, 8 * tile + 8)
                value = factors[0] * basis[0, plane, at]
                for i in range(1, j + 1):
                    value = value + factors[i] * basis[i, plane, at]
                made[j, plane, at] = value
        copy(j).start()

    alphas, betas = coefficients(gram, ready)
    for r, values in enumerate((alphas, betas)):
        table = jnp.zeros((8, 128), jnp.float32)
        for j, value in enumerate(values):
            table = jnp.where(lane == j, value, table)
        small[r : r + 1, :] = table[0:1, 0:ITERS]
    last = pltpu.make_async_copy(small, tridiagonal, done.at[COUNT])
    last.start()
    for j in range(COUNT):
        copy(j).wait()
    last.wait()


def call(kernel, out_shape, scratch=(), flops=10000, mebibytes=4, **specs):
    return pl.pallas_call(
        kernel,
        out_shape=out_shape,
        scratch_shapes=list(scratch),
        cost_estimate=pl.CostEstimate(flops=flops, bytes_accessed=flops, transcendentals=0),
        compiler_params=pltpu.CompilerParams(
            vmem_limit_bytes=mebibytes and mebibytes * 2**20
        ),
        interpret=INTERPRET,
        **specs,
    )


def to_rows(*pieces):
    return jnp.concatenate([p.reshape(-1, 128) for p in pieces])


def shards(v, p):
    f32 = jnp.float32

    def line(axis, step):
        n = lax.axis_size(axis)
        return [(i, i + step) for i in range(n) if 0 <= i + step < n]

    def exchange(to_next, to_previous, axis):
        return (
            lax.ppermute(to_next, axis, line(axis, 1)),
            lax.ppermute(to_previous, axis, line(axis, -1)),
        )

    halo = jax.ShapeDtypeStruct((9, 8, 128), f32)
    last, first = slice(24, 32), slice(0, 8)
    y_low, y_high = exchange(
        *call(edges_kernel, (halo, halo), mebibytes=1)(
            v[:, last], v[:, first], p[:, last], p[:, first]
        ),
        "py",
    )
    z_low, z_high = exchange(
        to_rows(v[3:], p[4:], y_low[4:8], y_high[4:8]),
        to_rows(v[:5], p[:4], y_low[:4], y_high[:4]),
        "pz",
    )
    blocks = (v, p, y_low, y_high, z_low, z_high)
    side = call(side_kernel, jax.ShapeDtypeStruct((88, 128), f32))(*blocks)
    side = lax.ppermute(side, "slab", [(0, 1), (1, 0)])
    n_z = lax.axis_size("pz")
    n_xy = lax.axis_size("slab") * lax.axis_size("py")
    block = [pltpu.VMEM((2, 18, 48, 128), f32)] * 5
    basis, rows = call(
        krylov_kernel,
        (jax.ShapeDtypeStruct((COUNT, 8, 32, 128), f32), jax.ShapeDtypeStruct((n_xy, 128), f32)),
        block + [pltpu.VMEM((8, 32, 128), f32), pltpu.VMEM((2, 16, 48, 128), f32)],
        20000000,
        12,
    )(*blocks, side)
    rows = lax.all_to_all(rows, ("slab", "py"), 0, 0, tiled=True)
    rows = call(rows_kernel, jax.ShapeDtypeStruct((n_z, 128), f32))(rows)
    rows = lax.all_to_all(rows, "pz", 0, 0, tiled=True)
    per_cell = 1.0 / (v.size * n_z * n_xy)
    return call(
        functools.partial(lanczos_kernel, per_cell),
        (
            jax.ShapeDtypeStruct((COUNT, 8, 32, 128), f32),
            jax.ShapeDtypeStruct((2, ITERS), f32),
        ),
        [
            pltpu.VMEM((COUNT, 8, 32, 128), f32),
            pltpu.VMEM((2, ITERS), f32),
            pltpu.SemaphoreType.DMA((COUNT + 1,)),
        ],
        flops=20000000,
        out_specs=(pl.BlockSpec(memory_space=pl.ANY),) * 2,
    )(rows, basis)


def solution(mesh):
    in_specs = (P("pz", "py", "slab"), P("pz", "py", "slab"))
    out_specs = (P(None, "pz", "py", "slab"), P())
    return jax.shard_map(shards, mesh=mesh, in_specs=in_specs, out_specs=out_specs, check_vma=False)
```

```python
import functools

import jax
import jax.numpy as jnp
from jax import lax
from jax.experimental import pallas as pl
from jax.experimental.pallas import tpu as pltpu
from jax.sharding import PartitionSpec as P

ITERS = 5
EPSILON = 1e-06
INTERPRET = False

SHIFTS = (0.75, 3.75, 13.25, 9.25, 5.25)
SCALE = 2.0**24
FIRST = 6.0 - SHIFTS[0]
COUNT = ITERS + 1
PAIRS = [(i, k) for i in range(COUNT) for k in range(i, COUNT)]


def two_sum(a, b):
    s = a + b
    t = s - a
    return s, (a - (s - t)) + (b - t)


def split(a):
    c = a * 4097.0
    high = c - (c - a)
    return high, a - high


def pair_add(a, b):
    s, e = two_sum(a[0], b[0])
    e = e + (a[1] + b[1])
    high = s + e
    return high, e - (high - s)


def pair_mul(a, b):
    p = a[0] * b[0]
    ah, al = split(a[0])
    bh, bl = split(b[0])
    e = ((ah * bh - p) + (ah * bl + al * bh)) + al * bl
    return p, e + (a[0] * b[1] + a[1] * b[0])


def pair_times(a, b):
    p = a[0] * b
    ah, al = split(a[0])
    bh, bl = split(b)
    e = ((ah * bh - p) + (ah * bl + al * bh)) + al * bl
    return p, e + a[1] * b


def pair_neg(a):
    return -a[0], -a[1]


def pair_sum(terms):
    terms = list(terms)
    while len(terms) > 1:
        rest = terms[len(terms) // 2 * 2 :]
        terms = [pair_add(terms[i], terms[i + 1]) for i in range(0, len(terms) - 1, 2)] + rest
    return terms[0]


def over_sublanes(a):
    for shift in (4, 2, 1):
        a = pair_add(a, (pltpu.roll(a[0], shift, 0), pltpu.roll(a[1], shift, 0)))
    return a


def lanes():
    return lax.broadcasted_iota(jnp.int32, (8, 128), 1)


def as_row(a):
    return jnp.where(lanes() < 64, a[0], pltpu.roll(a[1], 64, 1))


def sum_of_rows(ref):
    blocks = [ref[pl.ds(8 * r, 8), :] for r in range(ref.shape[0] // 8)]
    return over_sublanes(pair_sum([(b, pltpu.roll(b, 64, 1)) for b in blocks]))


def edges_kernel(v_last, v_first, p_last, p_first, to_next, to_previous):
    to_next[0:8, 0:3] = p_last[:, 5:8]
    to_next[0:8, 3:8] = v_last[:, 3:8]
    to_previous[0:8, 0:5] = v_first[:, 0:5]
    to_previous[0:8, 5:8] = p_first[:, 0:3]
    for plane in range(8):
        to_next[8, plane : plane + 1] = p_last[plane, 4:5]
        to_previous[8, plane : plane + 1] = p_first[plane, 3:4]


def blocks_of(refs):
    v, p, y_low, y_high, z_low, z_high = refs
    tiles = [(ref, (plane, pl.ds(8 * r, 8))) for ref in (v, p) for plane in range(8) for r in range(4)]
    tiles += [(ref, (plane, pl.ds(0, 8))) for ref in (y_low, y_high) for plane in range(9)]
    return tiles + [(ref, (pl.ds(8 * r, 8),)) for ref in (z_low, z_high) for r in range(44)]


def side_kernel(*refs):
    out = refs[-1]
    mine = lax.axis_index("slab")
    lane = lanes()
    tiles = blocks_of(refs[:-1])
    for start in range(0, len(tiles), 16):
        packed = jnp.zeros((8, 128), jnp.float32)
        for k, (ref, at) in enumerate(tiles[start : start + 16]):
            moved = pltpu.roll(ref[at], lax.rem(8 * k + 8 * (1 - mine), 128), 1)
            packed = jnp.where((lane >= 8 * k) & (lane < 8 * k + 8), moved, packed)
        out[start // 2 : start // 2 + 8] = packed


def assemble(tile_of, k0, dg, slot):
    row = lax.broadcasted_iota(jnp.int32, (8, 128), 0)

    def halo(tile, high, plane, fourth=None):
        rows = slice(40, 48) if high else slice(0, 8)
        k0[slot, plane, rows] = tile * SCALE
        near = pltpu.roll(tile, 3 if high else 5, 0)
        if fourth is not None:
            near = jnp.where(row == (3 if high else 4), jnp.broadcast_to(fourth, (8, 128)), near)
        dg[slot, plane - 1, rows] = near + FIRST

    def inner(ref, plane, r, value):
        ref[slot, plane, 8 + 8 * r : 16 + 8 * r] = value

    for plane in range(8):
        for r in range(4):
            inner(k0, 5 + plane, r, tile_of(4 * plane + r) * SCALE)
            inner(dg, 4 + plane, r, tile_of(32 + 4 * plane + r) + FIRST)
    for high in (0, 1):
        start = 64 + 9 * high
        fourths = tile_of(start + 8)
        for plane in range(8):
            halo(tile_of(start + plane), high, 5 + plane, fourths[plane : plane + 1])
    for side in (0, 1):
        start = 82 + 44 * side
        for plane in range(5):
            for r in range(4):
                inner(k0, (13 if side else 0) + plane, r, tile_of(start + 4 * plane + r) * SCALE)
        for plane in range(4):
            for r in range(4):
                value = tile_of(start + 20 + 4 * plane + r) + FIRST
                inner(dg, (12 if side else 0) + plane, r, value)
        for high in (0, 1):
            for plane in range(4):
                tile = tile_of(start + 36 + 4 * high + plane)
                halo(tile, high, (13 if side else 1) + plane)


def krylov_kernel(v, p, y_low, y_high, z_low, z_high, side, k_out, row_out, k0, k1, k2, k3, k4, k5, dg):
    mine = lax.axis_index("slab")
    y, z = lax.axis_index("py"), lax.axis_index("pz")
    inside = {
        "y_low": jnp.where(y > 0, 1.0, 0.0),
        "y_high": jnp.where(y < lax.axis_size("py") - 1, 1.0, 0.0),
        "z_low": jnp.where(z > 0, 1.0, 0.0),
        "z_high": jnp.where(z < lax.axis_size("pz") - 1, 1.0, 0.0),
    }
    lane = lax.broadcasted_iota(jnp.int32, (48, 128), 1)
    first, last = lane == 0, lane == 127
    near = (lane >= 120 * mine) & (lane < 8 + 120 * mine)
    near8 = near[0:8]
    tiles = blocks_of((v, p, y_low, y_high, z_low, z_high))

    def own_tile(n):
        ref, at = tiles[n]
        return ref[at]

    def other_tile(n):
        k = n % 16
        shift = lax.rem(120 * mine + 128 - 8 * k, 128)
        return jnp.where(near8, pltpu.roll(side[pl.ds(n // 16 * 8, 8), :], shift, 1), 0.0)

    assemble(own_tile, k0, dg, 0)
    assemble(other_tile, k0, dg, 1)
    basis = (k0, k1, k2, k3, k4, k5)
    for step in range(1, COUNT):
        old, new = basis[step - 1], basis[step]
        shift = SHIFTS[0] - SHIFTS[step - 1]
        for plane in range(step, 18 - step):
            away = max(5 - plane, plane - 12, 0)
            f = [old[t, plane] for t in (0, 1)]
            up = [pltpu.roll(a, 1, 1) for a in f]
            down = [pltpu.roll(a, 127, 1) for a in f]
            for t in (0, 1):
                reach = ITERS - step - t - away
                if reach < 0:
                    continue
                beside = jnp.where(first, up[1 - t], up[t]) + jnp.where(last, down[1 - t], down[t])
                rows = slice(0, 48) if reach > 0 else slice(8, 40)
                along_y = old[t, plane, 7:39] + old[t, plane, 9:41]
                if reach > 0:
                    along_y = jnp.concatenate(
                        [
                            pltpu.roll(f[t][0:8], 1, 0) + old[t, plane, 1:9],
                            along_y,
                            old[t, plane, 39:47] + pltpu.roll(f[t][40:48], 7, 0),
                        ]
                    )
                around = beside[rows] + along_y
                around = around + (old[t, plane - 1, rows] + old[t, plane + 1, rows])
                factor = dg[t, plane - 1, rows]
                if shift != 0.0:
                    factor = factor + shift
                image = factor * f[t][rows] - around
                if t == 1:
                    image = jnp.where(near[rows], image, 0.0)
                if step == ITERS:
                    new[plane - ITERS] = image
                    continue
                if plane < ITERS:
                    image = image * inside["z_low"]
                if plane >= 13:
                    image = image * inside["z_high"]
                if reach == 0:
                    new[t, plane, rows] = image
                    continue
                new[t, plane, 0:8] = image[0:8] * inside["y_low"]
                new[t, plane, 8:40] = image[8:40]
                new[t, plane, 40:48] = image[40:48] * inside["y_high"]
    sums = [None] * len(PAIRS)
    for plane in range(8):
        for tile in range(4):
            own = [b[0, 5 + plane, 8 + 8 * tile : 16 + 8 * tile] for b in basis[:ITERS]]
            own.append(k5[plane, 8 * tile : 8 + 8 * tile])
            for i, value in enumerate(own):
                k_out[i, plane, 8 * tile : 8 + 8 * tile] = value
            parts = [split(value) for value in own]
            for n, (i, k) in enumerate(PAIRS):
                big = parts[i][0] * parts[k][0]
                small = parts[i][0] * parts[k][1] + parts[i][1] * own[k]
                if sums[n] is None:
                    sums[n] = (big, small)
                else:
                    s, e = two_sum(sums[n][0], big)
                    sums[n] = (s, sums[n][1] + (e + small))
    row = lax.broadcasted_iota(jnp.int32, (8, 128), 0)
    tables = []
    sums = [over_sublanes(s) for s in sums]
    for half in (0, 1):
        blocks = []
        for start in range(0, len(PAIRS), 8):
            block = sums[start][half]
            for n in range(start + 1, min(start + 8, len(PAIRS))):
                block = jnp.where(row == n - start, sums[n][half], block)
            blocks.append(block)
        blocks.append(jnp.zeros((128 - 8 * len(blocks), 128), jnp.float32))
        tables.append(jnp.transpose(jnp.concatenate(blocks)))
    total = over_sublanes(
        pair_sum([tuple(t[8 * r : 8 * r + 8] for t in tables) for r in range(16)])
    )
    sent = as_row(total)
    for r in range(row_out.shape[0] // 8):
        row_out[8 * r : 8 * r + 8] = sent


def rows_kernel(rows, out):
    sent = as_row(sum_of_rows(rows))
    for r in range(out.shape[0] // 8):
        out[8 * r : 8 * r + 8] = sent


def root_of(square):
    x = pair_add(square, (jnp.full_like(square[0], EPSILON), jnp.zeros_like(square[0])))
    r = lax.rsqrt(x[0])
    r = r * (1.5 - (0.5 * x[0]) * (r * r))
    one = pair_times(pair_times(x, r), r)
    miss = (1.0 - one[0]) - one[1]
    return x[0] * r, (r, r * (0.5 * miss))


def row_of(a, i):
    return tuple(jnp.broadcast_to(t[i : i + 1, :], (8, 128)) for t in a)


def pair_dot(a, b):
    return over_sublanes(pair_mul(a, b))


def coefficients(gram, ready):
    row = lax.broadcasted_iota(jnp.int32, (8, 128), 0)
    zero = jnp.zeros((8, 128), jnp.float32)
    shifts = zero
    for i, shift in enumerate(SHIFTS):
        shifts = jnp.where(row == i, shift, shifts)
    _, inverse = root_of(tuple(g * SCALE**-2 for g in row_of(gram[0], 0)))
    columns = [(jnp.where(row == 0, 1.0, zero), zero)]
    sizes = [tuple(r / SCALE for r in inverse)]
    lack = [[(EPSILON * inverse[0]) * inverse[0]]]
    alphas, betas = [], []
    for j in range(ITERS):
        newest = columns[j]
        image = pair_add(
            pair_times(newest, shifts), tuple(pltpu.roll(t, 1, 0) for t in newest)
        )
        weights = pair_sum([pair_mul(gram[k], row_of(image, k)) for k in range(j + 2)])
        dots = [pair_dot(columns[k], weights) for k in range(j + 1)]
        norm = pair_dot(image, weights)
        ready(j, columns[j], sizes[j])
        first = [pair_mul(dots[k], sizes[k]) for k in range(j + 1)]
        second = [sum(lack[k][l] * first[l][0] for l in range(j + 1)) for k in range(j + 1)]
        third = [sum(lack[k][l] * second[l] for l in range(j + 1)) for k in range(j + 1)]
        both = [pair_add(first[k], (second[k], zero)) for k in range(j + 1)]
        rest = sum(
            second[k] * second[k] - both[k][0] * (second[k] + third[k]) for k in range(j + 1)
        )
        square = pair_sum(
            [norm] + [pair_neg(pair_mul(f, f)) for f in first] + [(rest, zero)]
        )
        square = pair_mul(square, pair_mul(sizes[j], sizes[j]))
        positive = square[0] + square[1] > 0.0
        beta, inverse = root_of(tuple(jnp.where(positive, s, 0.0) for s in square))
        alphas.append(both[j][0] * sizes[j][0])
        betas.append(beta)
        columns.append(
            pair_sum(
                [image]
                + [
                    pair_neg(pair_mul(columns[k], pair_mul(both[k], sizes[k])))
                    for k in range(j + 1)
                ]
            )
        )
        sizes.append(pair_mul(sizes[j], inverse))
        for k in range(j + 1):
            lack[k].append(-third[k] * sizes[j + 1][0])
        lack.append([lack[k][j + 1] for k in range(j + 1)] + [(EPSILON * inverse[0]) * inverse[0]])
    ready(ITERS, columns[ITERS], sizes[ITERS])
    return alphas, betas


def lanczos_kernel(per_cell, rows, basis, vectors, tridiagonal, made, small, done):
    total = sum_of_rows(rows)
    lane, row = lanes(), lax.broadcasted_iota(jnp.int32, (8, 128), 0)
    gram = []
    for k in range(COUNT):
        low, high = jnp.minimum(row, k), jnp.maximum(row, k)
        place = low * COUNT - ((low * (low - 1)) >> 1) + (high - low)
        picked = (lane == place) & (row < COUNT)
        gram.append(
            tuple(
                jnp.broadcast_to(
                    jnp.sum(jnp.where(picked, t, 0.0), axis=1, keepdims=True) * per_cell, (8, 128)
                )
                for t in total
            )
        )

    def copy(j):
        return pltpu.make_async_copy(made.at[j], vectors.at[j], done.at[j])

    def ready(j, column, size):
        scaled = pair_mul(column, size)
        scaled = scaled[0] + scaled[1]
        factors = [jnp.broadcast_to(scaled[i : i + 1, :], (8, 128)) for i in range(j + 1)]
        for plane in range(8):
            for tile in range(4):
                at = slice(8 * tile, 8 * tile + 8)
                value = factors[0] * basis[0, plane, at]
                for i in range(1, j + 1):
                    value = value + factors[i] * basis[i, plane, at]
                made[j, plane, at] = value
        copy(j).start()

    alphas, betas = coefficients(gram, ready)
    for r, values in enumerate((alphas, betas)):
        table = jnp.zeros((8, 128), jnp.float32)
        for j, value in enumerate(values):
            table = jnp.where(lane == j, value, table)
        small[r : r + 1, :] = table[0:1, 0:ITERS]
    last = pltpu.make_async_copy(small, tridiagonal, done.at[COUNT])
    last.start()
    for j in range(COUNT):
        copy(j).wait()
    last.wait()


def call(kernel, out_shape, scratch=(), flops=10000, mebibytes=4, **specs):
    return pl.pallas_call(
        kernel,
        out_shape=out_shape,
        scratch_shapes=list(scratch),
        cost_estimate=pl.CostEstimate(flops=flops, bytes_accessed=flops, transcendentals=0),
        compiler_params=pltpu.CompilerParams(
            vmem_limit_bytes=mebibytes and mebibytes * 2**20
        ),
        interpret=INTERPRET,
        **specs,
    )


def to_rows(*pieces):
    return jnp.concatenate([p.reshape(-1, 128) for p in pieces])


def shards(v, p):
    f32 = jnp.float32

    def line(axis, step):
        n = lax.axis_size(axis)
        return [(i, i + step) for i in range(n) if 0 <= i + step < n]

    def exchange(to_next, to_previous, axis):
        return (
            lax.ppermute(to_next, axis, line(axis, 1)),
            lax.ppermute(to_previous, axis, line(axis, -1)),
        )

    halo = jax.ShapeDtypeStruct((9, 8, 128), f32)
    last, first = slice(24, 32), slice(0, 8)
    y_low, y_high = exchange(
        *call(edges_kernel, (halo, halo), mebibytes=1)(
            v[:, last], v[:, first], p[:, last], p[:, first]
        ),
        "py",
    )
    z_low, z_high = exchange(
        to_rows(v[3:], p[4:], y_low[4:8], y_high[4:8]),
        to_rows(v[:5], p[:4], y_low[:4], y_high[:4]),
        "pz",
    )
    blocks = (v, p, y_low, y_high, z_low, z_high)
    side = call(side_kernel, jax.ShapeDtypeStruct((88, 128), f32))(*blocks)
    side = lax.ppermute(side, "slab", [(0, 1), (1, 0)])
    n_z = lax.axis_size("pz")
    n_xy = lax.axis_size("slab") * lax.axis_size("py")
    block = [pltpu.VMEM((2, 18, 48, 128), f32)] * 5
    basis, rows = call(
        krylov_kernel,
        (jax.ShapeDtypeStruct((COUNT, 8, 32, 128), f32), jax.ShapeDtypeStruct((n_xy, 128), f32)),
        block + [pltpu.VMEM((8, 32, 128), f32), pltpu.VMEM((2, 16, 48, 128), f32)],
        20000000,
        12,
    )(*blocks, side)
    rows = lax.all_to_all(rows, ("py", "slab"), 0, 0, tiled=True)
    rows = call(rows_kernel, jax.ShapeDtypeStruct((n_z, 128), f32))(rows)
    rows = lax.all_to_all(rows, "pz", 0, 0, tiled=True)
    per_cell = 1.0 / (v.size * n_z * n_xy)
    return call(
        functools.partial(lanczos_kernel, per_cell),
        (
            jax.ShapeDtypeStruct((COUNT, 8, 32, 128), f32),
            jax.ShapeDtypeStruct((2, ITERS), f32),
        ),
        [
            pltpu.VMEM((COUNT, 8, 32, 128), f32),
            pltpu.VMEM((2, ITERS), f32),
            pltpu.SemaphoreType.DMA((COUNT + 1,)),
        ],
        flops=20000000,
        out_specs=(pl.BlockSpec(memory_space=pl.ANY),) * 2,
    )(rows, basis)


def solution(mesh):
    in_specs = (P("pz", "py", "slab"), P("pz", "py", "slab"))
    out_specs = (P(None, "pz", "py", "slab"), P())
    return jax.shard_map(shards, mesh=mesh, in_specs=in_specs, out_specs=out_specs, check_vma=False)
```

```python
import functools

import jax
import jax.numpy as jnp
from jax import lax
from jax.experimental import pallas as pl
from jax.experimental.pallas import tpu as pltpu
from jax.sharding import PartitionSpec as P

ITERS = 5
EPSILON = 1e-06
INTERPRET = False

SHIFTS = (0.75, 3.75, 13.25, 9.25, 5.25)
SCALE = 2.0**24
FIRST = 6.0 - SHIFTS[0]
COUNT = ITERS + 1
PAIRS = [(i, k) for i in range(COUNT) for k in range(i, COUNT)]


def two_sum(a, b):
    s = a + b
    t = s - a
    return s, (a - (s - t)) + (b - t)


def split(a):
    c = a * 4097.0
    high = c - (c - a)
    return high, a - high


def pair_add(a, b):
    s, e = two_sum(a[0], b[0])
    e = e + (a[1] + b[1])
    high = s + e
    return high, e - (high - s)


def pair_mul(a, b):
    p = a[0] * b[0]
    ah, al = split(a[0])
    bh, bl = split(b[0])
    e = ((ah * bh - p) + (ah * bl + al * bh)) + al * bl
    return p, e + (a[0] * b[1] + a[1] * b[0])


def pair_times(a, b):
    p = a[0] * b
    ah, al = split(a[0])
    bh, bl = split(b)
    e = ((ah * bh - p) + (ah * bl + al * bh)) + al * bl
    return p, e + a[1] * b


def pair_neg(a):
    return -a[0], -a[1]


def pair_sum(terms):
    terms = list(terms)
    while len(terms) > 1:
        rest = terms[len(terms) // 2 * 2 :]
        terms = [pair_add(terms[i], terms[i + 1]) for i in range(0, len(terms) - 1, 2)] + rest
    return terms[0]


def over_sublanes(a):
    for shift in (4, 2, 1):
        a = pair_add(a, (pltpu.roll(a[0], shift, 0), pltpu.roll(a[1], shift, 0)))
    return a


def lanes():
    return lax.broadcasted_iota(jnp.int32, (8, 128), 1)


def as_row(a):
    return jnp.where(lanes() < 64, a[0], pltpu.roll(a[1], 64, 1))


def sum_of_rows(ref):
    blocks = [ref[pl.ds(8 * r, 8), :] for r in range(ref.shape[0] // 8)]
    return over_sublanes(pair_sum([(b, pltpu.roll(b, 64, 1)) for b in blocks]))


def edges_kernel(v_last, v_first, p_last, p_first, to_next, to_previous):
    to_next[0:8, 0:3] = p_last[:, 5:8]
    to_next[0:8, 3:8] = v_last[:, 3:8]
    to_previous[0:8, 0:5] = v_first[:, 0:5]
    to_previous[0:8, 5:8] = p_first[:, 0:3]
    for plane in range(8):
        to_next[8, plane : plane + 1] = p_last[plane, 4:5]
        to_previous[8, plane : plane + 1] = p_first[plane, 3:4]


def blocks_of(refs):
    v, p, y_low, y_high, z_low, z_high = refs
    tiles = [(ref, (plane, pl.ds(8 * r, 8))) for ref in (v, p) for plane in range(8) for r in range(4)]
    tiles += [(ref, (plane, pl.ds(0, 8))) for ref in (y_low, y_high) for plane in range(9)]
    return tiles + [(ref, (pl.ds(8 * r, 8),)) for ref in (z_low, z_high) for r in range(44)]


def side_kernel(*refs):
    out = refs[-1]
    mine = lax.axis_index("slab")
    lane = lanes()
    tiles = blocks_of(refs[:-1])
    for start in range(0, len(tiles), 16):
        packed = jnp.zeros((8, 128), jnp.float32)
        for k, (ref, at) in enumerate(tiles[start : start + 16]):
            moved = pltpu.roll(ref[at], lax.rem(8 * k + 8 * (1 - mine), 128), 1)
            packed = jnp.where((lane >= 8 * k) & (lane < 8 * k + 8), moved, packed)
        out[start // 2 : start // 2 + 8] = packed


def assemble(tile_of, k0, dg, slot):
    row = lax.broadcasted_iota(jnp.int32, (8, 128), 0)

    def halo(tile, high, plane, fourth=None):
        rows = slice(40, 48) if high else slice(0, 8)
        k0[slot, plane, rows] = tile * SCALE
        near = pltpu.roll(tile, 3 if high else 5, 0)
        if fourth is not None:
            near = jnp.where(row == (3 if high else 4), jnp.broadcast_to(fourth, (8, 128)), near)
        dg[slot, plane - 1, rows] = near + FIRST

    def inner(ref, plane, r, value):
        ref[slot, plane, 8 + 8 * r : 16 + 8 * r] = value

    for plane in range(8):
        for r in range(4):
            inner(k0, 5 + plane, r, tile_of(4 * plane + r) * SCALE)
            inner(dg, 4 + plane, r, tile_of(32 + 4 * plane + r) + FIRST)
    for high in (0, 1):
        start = 64 + 9 * high
        fourths = tile_of(start + 8)
        for plane in range(8):
            halo(tile_of(start + plane), high, 5 + plane, fourths[plane : plane + 1])
    for side in (0, 1):
        start = 82 + 44 * side
        for plane in range(5):
            for r in range(4):
                inner(k0, (13 if side else 0) + plane, r, tile_of(start + 4 * plane + r) * SCALE)
        for plane in range(4):
            for r in range(4):
                value = tile_of(start + 20 + 4 * plane + r) + FIRST
                inner(dg, (12 if side else 0) + plane, r, value)
        for high in (0, 1):
            for plane in range(4):
                tile = tile_of(start + 36 + 4 * high + plane)
                halo(tile, high, (13 if side else 1) + plane)


def krylov_kernel(v, p, y_low, y_high, z_low, z_high, side, k_out, row_out, k0, k1, k2, k3, k4, k5, dg):
    mine = lax.axis_index("slab")
    y, z = lax.axis_index("py"), lax.axis_index("pz")
    inside = {
        "y_low": jnp.where(y > 0, 1.0, 0.0),
        "y_high": jnp.where(y < lax.axis_size("py") - 1, 1.0, 0.0),
        "z_low": jnp.where(z > 0, 1.0, 0.0),
        "z_high": jnp.where(z < lax.axis_size("pz") - 1, 1.0, 0.0),
    }
    lane = lax.broadcasted_iota(jnp.int32, (48, 128), 1)
    first, last = lane == 0, lane == 127
    near = (lane >= 120 * mine) & (lane < 8 + 120 * mine)
    near8 = near[0:8]
    tiles = blocks_of((v, p, y_low, y_high, z_low, z_high))

    def own_tile(n):
        ref, at = tiles[n]
        return ref[at]

    def other_tile(n):
        k = n % 16
        shift = lax.rem(120 * mine + 128 - 8 * k, 128)
        return jnp.where(near8, pltpu.roll(side[pl.ds(n // 16 * 8, 8), :], shift, 1), 0.0)

    assemble(own_tile, k0, dg, 0)
    assemble(other_tile, k0, dg, 1)
    basis = (k0, k1, k2, k3, k4, k5)
    for step in range(1, COUNT):
        old, new = basis[step - 1], basis[step]
        shift = SHIFTS[0] - SHIFTS[step - 1]
        for plane in range(step, 18 - step):
            away = max(5 - plane, plane - 12, 0)
            f = [old[t, plane] for t in (0, 1)]
            up = [pltpu.roll(a, 1, 1) for a in f]
            down = [pltpu.roll(a, 127, 1) for a in f]
            for t in (0, 1):
                reach = ITERS - step - t - away
                if reach < 0:
                    continue
                beside = jnp.where(first, up[1 - t], up[t]) + jnp.where(last, down[1 - t], down[t])
                rows = slice(0, 48) if reach > 0 else slice(8, 40)
                along_y = old[t, plane, 7:39] + old[t, plane, 9:41]
                if reach > 0:
                    along_y = jnp.concatenate(
                        [
                            pltpu.roll(f[t][0:8], 1, 0) + old[t, plane, 1:9],
                            along_y,
                            old[t, plane, 39:47] + pltpu.roll(f[t][40:48], 7, 0),
                        ]
                    )
                around = beside[rows] + along_y
                around = around + (old[t, plane - 1, rows] + old[t, plane + 1, rows])
                factor = dg[t, plane - 1, rows]
                if shift != 0.0:
                    factor = factor + shift
                image = factor * f[t][rows] - around
                if t == 1:
                    image = jnp.where(near[rows], image, 0.0)
                if step == ITERS:
                    new[plane - ITERS] = image
                    continue
                if plane < ITERS:
                    image = image * inside["z_low"]
                if plane >= 13:
                    image = image * inside["z_high"]
                if reach == 0:
                    new[t, plane, rows] = image
                    continue
                new[t, plane, 0:8] = image[0:8] * inside["y_low"]
                new[t, plane, 8:40] = image[8:40]
                new[t, plane, 40:48] = image[40:48] * inside["y_high"]
    sums = [None] * len(PAIRS)
    for plane in range(8):
        for tile in range(4):
            own = [b[0, 5 + plane, 8 + 8 * tile : 16 + 8 * tile] for b in basis[:ITERS]]
            own.append(k5[plane, 8 * tile : 8 + 8 * tile])
            for i, value in enumerate(own):
                k_out[i, plane, 8 * tile : 8 + 8 * tile] = value
            parts = [split(value) for value in own]
            for n, (i, k) in enumerate(PAIRS):
                big = parts[i][0] * parts[k][0]
                small = parts[i][0] * parts[k][1] + parts[i][1] * own[k]
                if sums[n] is None:
                    sums[n] = (big, small)
                else:
                    s, e = two_sum(sums[n][0], big)
                    sums[n] = (s, sums[n][1] + (e + small))
    row = lax.broadcasted_iota(jnp.int32, (8, 128), 0)
    tables = []
    sums = [over_sublanes(s) for s in sums]
    for half in (0, 1):
        blocks = []
        for start in range(0, len(PAIRS), 8):
            block = sums[start][half]
            for n in range(start + 1, min(start + 8, len(PAIRS))):
                block = jnp.where(row == n - start, sums[n][half], block)
            blocks.append(block)
        blocks.append(jnp.zeros((128 - 8 * len(blocks), 128), jnp.float32))
        tables.append(jnp.transpose(jnp.concatenate(blocks)))
    total = over_sublanes(
        pair_sum([tuple(t[8 * r : 8 * r + 8] for t in tables) for r in range(16)])
    )
    sent = as_row(total)
    for r in range(row_out.shape[0] // 8):
        row_out[8 * r : 8 * r + 8] = sent


def rows_kernel(rows, out):
    sent = as_row(sum_of_rows(rows))
    for r in range(out.shape[0] // 8):
        out[8 * r : 8 * r + 8] = sent


def root_of(square):
    x = pair_add(square, (jnp.full_like(square[0], EPSILON), jnp.zeros_like(square[0])))
    r = lax.rsqrt(x[0])
    r = r * (1.5 - (0.5 * x[0]) * (r * r))
    one = pair_times(pair_times(x, r), r)
    miss = (1.0 - one[0]) - one[1]
    return x[0] * r, (r, r * (0.5 * miss))


def row_of(a, i):
    return tuple(jnp.broadcast_to(t[i : i + 1, :], (8, 128)) for t in a)


def pair_dot(a, b):
    return over_sublanes(pair_mul(a, b))


def coefficients(gram, ready):
    row = lax.broadcasted_iota(jnp.int32, (8, 128), 0)
    zero = jnp.zeros((8, 128), jnp.float32)
    shifts = zero
    for i, shift in enumerate(SHIFTS):
        shifts = jnp.where(row == i, shift, shifts)
    _, inverse = root_of(tuple(g * SCALE**-2 for g in row_of(gram[0], 0)))
    columns = [(jnp.where(row == 0, 1.0, zero), zero)]
    sizes = [tuple(r / SCALE for r in inverse)]
    lack = [[(EPSILON * inverse[0]) * inverse[0]]]
    alphas, betas = [], []
    for j in range(ITERS):
        newest = columns[j]
        image = pair_add(
            pair_times(newest, shifts), tuple(pltpu.roll(t, 1, 0) for t in newest)
        )
        weights = pair_sum([pair_mul(gram[k], row_of(image, k)) for k in range(j + 2)])
        dots = [pair_dot(columns[k], weights) for k in range(j + 1)]
        norm = pair_dot(image, weights)
        ready(j, columns[j], sizes[j])
        first = [pair_mul(dots[k], sizes[k]) for k in range(j + 1)]
        second = [sum(lack[k][l] * first[l][0] for l in range(j + 1)) for k in range(j + 1)]
        third = [sum(lack[k][l] * second[l] for l in range(j + 1)) for k in range(j + 1)]
        both = [pair_add(first[k], (second[k], zero)) for k in range(j + 1)]
        rest = sum(
            second[k] * second[k] - both[k][0] * (second[k] + third[k]) for k in range(j + 1)
        )
        square = pair_sum(
            [norm] + [pair_neg(pair_mul(f, f)) for f in first] + [(rest, zero)]
        )
        square = pair_mul(square, pair_mul(sizes[j], sizes[j]))
        positive = square[0] + square[1] > 0.0
        beta, inverse = root_of(tuple(jnp.where(positive, s, 0.0) for s in square))
        alphas.append(both[j][0] * sizes[j][0])
        betas.append(beta)
        columns.append(
            pair_sum(
                [image]
                + [
                    pair_neg(pair_mul(columns[k], pair_mul(both[k], sizes[k])))
                    for k in range(j + 1)
                ]
            )
        )
        sizes.append(pair_mul(sizes[j], inverse))
        for k in range(j + 1):
            lack[k].append(-third[k] * sizes[j + 1][0])
        lack.append([lack[k][j + 1] for k in range(j + 1)] + [(EPSILON * inverse[0]) * inverse[0]])
    ready(ITERS, columns[ITERS], sizes[ITERS])
    return alphas, betas


def lanczos_kernel(per_cell, rows, basis, vectors, tridiagonal, made, small, done):
    total = sum_of_rows(rows)
    lane, row = lanes(), lax.broadcasted_iota(jnp.int32, (8, 128), 0)
    gram = []
    for k in range(COUNT):
        low, high = jnp.minimum(row, k), jnp.maximum(row, k)
        place = low * COUNT - ((low * (low - 1)) >> 1) + (high - low)
        picked = (lane == place) & (row < COUNT)
        gram.append(
            tuple(
                jnp.broadcast_to(
                    jnp.sum(jnp.where(picked, t, 0.0), axis=1, keepdims=True) * per_cell, (8, 128)
                )
                for t in total
            )
        )

    def copy(j):
        return pltpu.make_async_copy(made.at[j], vectors.at[j], done.at[j])

    def ready(j, column, size):
        scaled = pair_mul(column, size)
        scaled = scaled[0] + scaled[1]
        factors = [jnp.broadcast_to(scaled[i : i + 1, :], (8, 128)) for i in range(j + 1)]
        for plane in range(8):
            for tile in range(4):
                at = slice(8 * tile, 8 * tile + 8)
                value = factors[0] * basis[0, plane, at]
                for i in range(1, j + 1):
                    value = value + factors[i] * basis[i, plane, at]
                made[j, plane, at] = value
        copy(j).start()

    alphas, betas = coefficients(gram, ready)
    for r, values in enumerate((alphas, betas)):
        table = jnp.zeros((8, 128), jnp.float32)
        for j, value in enumerate(values):
            table = jnp.where(lane == j, value, table)
        small[r : r + 1, :] = table[0:1, 0:ITERS]
    last = pltpu.make_async_copy(small, tridiagonal, done.at[COUNT])
    last.start()
    for j in range(COUNT):
        copy(j).wait()
    last.wait()


def call(kernel, out_shape, scratch=(), flops=10000, mebibytes=4, **specs):
    return pl.pallas_call(
        kernel,
        out_shape=out_shape,
        scratch_shapes=list(scratch),
        cost_estimate=pl.CostEstimate(flops=flops, bytes_accessed=flops, transcendentals=0),
        compiler_params=pltpu.CompilerParams(
            vmem_limit_bytes=mebibytes and mebibytes * 2**20
        ),
        interpret=INTERPRET,
        **specs,
    )


def to_rows(*pieces):
    return jnp.concatenate([p.reshape(-1, 128) for p in pieces])


def shards(v, p):
    f32 = jnp.float32

    def exchange(to_next, to_previous, axis):
        n = lax.axis_size(axis)
        even = lax.axis_index(axis) % 2 == 0

        def swapped(value, start):
            pairs = [(i, i + 1) for i in range(start, n - 1, 2)]
            return lax.ppermute(value, axis, pairs + [(k, i) for i, k in pairs])

        a = swapped(jnp.where(even, to_next, to_previous), 0)
        b = swapped(jnp.where(even, to_previous, to_next), 1)
        return jnp.where(even, b, a), jnp.where(even, a, b)

    halo = jax.ShapeDtypeStruct((9, 8, 128), f32)
    last, first = slice(24, 32), slice(0, 8)
    y_low, y_high = exchange(
        *call(edges_kernel, (halo, halo), mebibytes=1)(
            v[:, last], v[:, first], p[:, last], p[:, first]
        ),
        "py",
    )
    z_low, z_high = exchange(
        to_rows(v[3:], p[4:], y_low[4:8], y_high[4:8]),
        to_rows(v[:5], p[:4], y_low[:4], y_high[:4]),
        "pz",
    )
    blocks = (v, p, y_low, y_high, z_low, z_high)
    side = call(side_kernel, jax.ShapeDtypeStruct((88, 128), f32))(*blocks)
    side = lax.ppermute(side, "slab", [(0, 1), (1, 0)])
    n_z = lax.axis_size("pz")
    n_xy = lax.axis_size("slab") * lax.axis_size("py")
    block = [pltpu.VMEM((2, 18, 48, 128), f32)] * 5
    basis, rows = call(
        krylov_kernel,
        (jax.ShapeDtypeStruct((COUNT, 8, 32, 128), f32), jax.ShapeDtypeStruct((n_xy, 128), f32)),
        block + [pltpu.VMEM((8, 32, 128), f32), pltpu.VMEM((2, 16, 48, 128), f32)],
        20000000,
        12,
    )(*blocks, side)
    rows = lax.all_to_all(rows, ("py", "slab"), 0, 0, tiled=True)
    rows = call(rows_kernel, jax.ShapeDtypeStruct((n_z, 128), f32))(rows)
    rows = lax.all_to_all(rows, "pz", 0, 0, tiled=True)
    per_cell = 1.0 / (v.size * n_z * n_xy)
    return call(
        functools.partial(lanczos_kernel, per_cell),
        (
            jax.ShapeDtypeStruct((COUNT, 8, 32, 128), f32),
            jax.ShapeDtypeStruct((2, ITERS), f32),
        ),
        [
            pltpu.VMEM((COUNT, 8, 32, 128), f32),
            pltpu.VMEM((2, ITERS), f32),
            pltpu.SemaphoreType.DMA((COUNT + 1,)),
        ],
        flops=20000000,
        out_specs=(pl.BlockSpec(memory_space=pl.ANY),) * 2,
    )(rows, basis)


def solution(mesh):
    in_specs = (P("pz", "py", "slab"), P("pz", "py", "slab"))
    out_specs = (P(None, "pz", "py", "slab"), P())
    return jax.shard_map(shards, mesh=mesh, in_specs=in_specs, out_specs=out_specs, check_vma=False)
```

```python
import functools

import jax
import jax.numpy as jnp
from jax import lax
from jax.experimental import pallas as pl
from jax.experimental.pallas import tpu as pltpu
from jax.sharding import PartitionSpec as P

ITERS = 5
EPSILON = 1e-06
INTERPRET = False

SHIFTS = (0.75, 3.75, 13.25, 9.25, 5.25)
SCALE = 2.0**24
FIRST = 6.0 - SHIFTS[0]
COUNT = ITERS + 1
PAIRS = [(i, k) for i in range(COUNT) for k in range(i, COUNT)]


def two_sum(a, b):
    s = a + b
    t = s - a
    return s, (a - (s - t)) + (b - t)


def split(a):
    c = a * 4097.0
    high = c - (c - a)
    return high, a - high


def pair_add(a, b):
    s, e = two_sum(a[0], b[0])
    e = e + (a[1] + b[1])
    high = s + e
    return high, e - (high - s)


def pair_mul(a, b):
    p = a[0] * b[0]
    ah, al = split(a[0])
    bh, bl = split(b[0])
    e = ((ah * bh - p) + (ah * bl + al * bh)) + al * bl
    return p, e + (a[0] * b[1] + a[1] * b[0])


def pair_times(a, b):
    p = a[0] * b
    ah, al = split(a[0])
    bh, bl = split(b)
    e = ((ah * bh - p) + (ah * bl + al * bh)) + al * bl
    return p, e + a[1] * b


def pair_neg(a):
    return -a[0], -a[1]


def pair_sum(terms):
    terms = list(terms)
    while len(terms) > 1:
        rest = terms[len(terms) // 2 * 2 :]
        terms = [pair_add(terms[i], terms[i + 1]) for i in range(0, len(terms) - 1, 2)] + rest
    return terms[0]


def over_sublanes(a):
    for shift in (4, 2, 1):
        a = pair_add(a, (pltpu.roll(a[0], shift, 0), pltpu.roll(a[1], shift, 0)))
    return a


def lanes():
    return lax.broadcasted_iota(jnp.int32, (8, 128), 1)


def as_row(a):
    return jnp.where(lanes() < 64, a[0], pltpu.roll(a[1], 64, 1))


def sum_of_rows(ref):
    blocks = [ref[pl.ds(8 * r, 8), :] for r in range(ref.shape[0] // 8)]
    return over_sublanes(pair_sum([(b, pltpu.roll(b, 64, 1)) for b in blocks]))


def edges_kernel(v_last, v_first, p_last, p_first, to_next, to_previous):
    to_next[0:8, 0:3] = p_last[:, 5:8]
    to_next[0:8, 3:8] = v_last[:, 3:8]
    to_previous[0:8, 0:5] = v_first[:, 0:5]
    to_previous[0:8, 5:8] = p_first[:, 0:3]
    for plane in range(8):
        to_next[8, plane : plane + 1] = p_last[plane, 4:5]
        to_previous[8, plane : plane + 1] = p_first[plane, 3:4]


def blocks_of(refs):
    v, p, y_low, y_high, z_low, z_high = refs
    tiles = [(ref, (plane, pl.ds(8 * r, 8))) for ref in (v, p) for plane in range(8) for r in range(4)]
    tiles += [(ref, (plane, pl.ds(0, 8))) for ref in (y_low, y_high) for plane in range(9)]
    return tiles + [(ref, (pl.ds(8 * r, 8),)) for ref in (z_low, z_high) for r in range(44)]


def side_kernel(*refs):
    out = refs[-1]
    mine = lax.axis_index("slab")
    lane = lanes()
    tiles = blocks_of(refs[:-1])
    for start in range(0, len(tiles), 16):
        packed = jnp.zeros((8, 128), jnp.float32)
        for k, (ref, at) in enumerate(tiles[start : start + 16]):
            moved = pltpu.roll(ref[at], lax.rem(8 * k + 8 * (1 - mine), 128), 1)
            packed = jnp.where((lane >= 8 * k) & (lane < 8 * k + 8), moved, packed)
        out[start // 2 : start // 2 + 8] = packed


def assemble(tile_of, k0, dg, slot):
    row = lax.broadcasted_iota(jnp.int32, (8, 128), 0)

    def halo(tile, high, plane, fourth=None):
        rows = slice(40, 48) if high else slice(0, 8)
        k0[slot, plane, rows] = tile * SCALE
        near = pltpu.roll(tile, 3 if high else 5, 0)
        if fourth is not None:
            near = jnp.where(row == (3 if high else 4), jnp.broadcast_to(fourth, (8, 128)), near)
        dg[slot, plane - 1, rows] = near + FIRST

    def inner(ref, plane, r, value):
        ref[slot, plane, 8 + 8 * r : 16 + 8 * r] = value

    for plane in range(8):
        for r in range(4):
            inner(k0, 5 + plane, r, tile_of(4 * plane + r) * SCALE)
            inner(dg, 4 + plane, r, tile_of(32 + 4 * plane + r) + FIRST)
    for high in (0, 1):
        start = 64 + 9 * high
        fourths = tile_of(start + 8)
        for plane in range(8):
            halo(tile_of(start + plane), high, 5 + plane, fourths[plane : plane + 1])
    for side in (0, 1):
        start = 82 + 44 * side
        for plane in range(5):
            for r in range(4):
                inner(k0, (13 if side else 0) + plane, r, tile_of(start + 4 * plane + r) * SCALE)
        for plane in range(4):
            for r in range(4):
                value = tile_of(start + 20 + 4 * plane + r) + FIRST
                inner(dg, (12 if side else 0) + plane, r, value)
        for high in (0, 1):
            for plane in range(4):
                tile = tile_of(start + 36 + 4 * high + plane)
                halo(tile, high, (13 if side else 1) + plane)


def krylov_kernel(v, p, y_low, y_high, z_low, z_high, side, k_out, row_out, k0, k1, k2, k3, k4, k5, dg):
    mine = lax.axis_index("slab")
    y, z = lax.axis_index("py"), lax.axis_index("pz")
    inside = {
        "y_low": jnp.where(y > 0, 1.0, 0.0),
        "y_high": jnp.where(y < lax.axis_size("py") - 1, 1.0, 0.0),
        "z_low": jnp.where(z > 0, 1.0, 0.0),
        "z_high": jnp.where(z < lax.axis_size("pz") - 1, 1.0, 0.0),
    }
    lane = lax.broadcasted_iota(jnp.int32, (48, 128), 1)
    first, last = lane == 0, lane == 127
    near = (lane >= 120 * mine) & (lane < 8 + 120 * mine)
    near8 = near[0:8]
    tiles = blocks_of((v, p, y_low, y_high, z_low, z_high))

    def own_tile(n):
        ref, at = tiles[n]
        return ref[at]

    def other_tile(n):
        k = n % 16
        shift = lax.rem(120 * mine + 128 - 8 * k, 128)
        return jnp.where(near8, pltpu.roll(side[pl.ds(n // 16 * 8, 8), :], shift, 1), 0.0)

    assemble(own_tile, k0, dg, 0)
    assemble(other_tile, k0, dg, 1)
    basis = (k0, k1, k2, k3, k4, k5)
    for step in range(1, COUNT):
        old, new = basis[step - 1], basis[step]
        shift = SHIFTS[0] - SHIFTS[step - 1]
        for plane in range(step, 18 - step):
            away = max(5 - plane, plane - 12, 0)
            f = [old[t, plane] for t in (0, 1)]
            up = [pltpu.roll(a, 1, 1) for a in f]
            down = [pltpu.roll(a, 127, 1) for a in f]
            for t in (0, 1):
                reach = ITERS - step - t - away
                if reach < 0:
                    continue
                beside = jnp.where(first, up[1 - t], up[t]) + jnp.where(last, down[1 - t], down[t])
                rows = slice(0, 48) if reach > 0 else slice(8, 40)
                along_y = old[t, plane, 7:39] + old[t, plane, 9:41]
                if reach > 0:
                    along_y = jnp.concatenate(
                        [
                            pltpu.roll(f[t][0:8], 1, 0) + old[t, plane, 1:9],
                            along_y,
                            old[t, plane, 39:47] + pltpu.roll(f[t][40:48], 7, 0),
                        ]
                    )
                around = beside[rows] + along_y
                around = around + (old[t, plane - 1, rows] + old[t, plane + 1, rows])
                factor = dg[t, plane - 1, rows]
                if shift != 0.0:
                    factor = factor + shift
                image = factor * f[t][rows] - around
                if t == 1:
                    image = jnp.where(near[rows], image, 0.0)
                if step == ITERS:
                    new[plane - ITERS] = image
                    continue
                if plane < ITERS:
                    image = image * inside["z_low"]
                if plane >= 13:
                    image = image * inside["z_high"]
                if reach == 0:
                    new[t, plane, rows] = image
                    continue
                new[t, plane, 0:8] = image[0:8] * inside["y_low"]
                new[t, plane, 8:40] = image[8:40]
                new[t, plane, 40:48] = image[40:48] * inside["y_high"]
    sums = [None] * len(PAIRS)
    for plane in range(8):
        for tile in range(4):
            own = [b[0, 5 + plane, 8 + 8 * tile : 16 + 8 * tile] for b in basis[:ITERS]]
            own.append(k5[plane, 8 * tile : 8 + 8 * tile])
            for i, value in enumerate(own):
                k_out[i, plane, 8 * tile : 8 + 8 * tile] = value
            parts = [split(value) for value in own]
            for n, (i, k) in enumerate(PAIRS):
                big = parts[i][0] * parts[k][0]
                small = parts[i][0] * parts[k][1] + parts[i][1] * own[k]
                if sums[n] is None:
                    sums[n] = (big, small)
                else:
                    s, e = two_sum(sums[n][0], big)
                    sums[n] = (s, sums[n][1] + (e + small))
    row = lax.broadcasted_iota(jnp.int32, (8, 128), 0)
    tables = []
    sums = [over_sublanes(s) for s in sums]
    for half in (0, 1):
        blocks = []
        for start in range(0, len(PAIRS), 8):
            block = sums[start][half]
            for n in range(start + 1, min(start + 8, len(PAIRS))):
                block = jnp.where(row == n - start, sums[n][half], block)
            blocks.append(block)
        blocks.append(jnp.zeros((128 - 8 * len(blocks), 128), jnp.float32))
        tables.append(jnp.transpose(jnp.concatenate(blocks)))
    total = over_sublanes(
        pair_sum([tuple(t[8 * r : 8 * r + 8] for t in tables) for r in range(16)])
    )
    sent = as_row(total)
    for r in range(row_out.shape[0] // 8):
        row_out[8 * r : 8 * r + 8] = sent


def rows_kernel(rows, out):
    sent = as_row(sum_of_rows(rows))
    for r in range(out.shape[0] // 8):
        out[8 * r : 8 * r + 8] = sent


def root_of(square):
    x = pair_add(square, (jnp.full_like(square[0], EPSILON), jnp.zeros_like(square[0])))
    r = lax.rsqrt(x[0])
    r = r * (1.5 - (0.5 * x[0]) * (r * r))
    one = pair_times(pair_times(x, r), r)
    miss = (1.0 - one[0]) - one[1]
    return x[0] * r, (r, r * (0.5 * miss))


def row_of(a, i):
    return tuple(jnp.broadcast_to(t[i : i + 1, :], (8, 128)) for t in a)


def pair_dot(a, b):
    return over_sublanes(pair_mul(a, b))


def coefficients(gram, ready):
    row = lax.broadcasted_iota(jnp.int32, (8, 128), 0)
    zero = jnp.zeros((8, 128), jnp.float32)
    shifts = zero
    for i, shift in enumerate(SHIFTS):
        shifts = jnp.where(row == i, shift, shifts)
    _, inverse = root_of(tuple(g * SCALE**-2 for g in row_of(gram[0], 0)))
    columns = [(jnp.where(row == 0, 1.0, zero), zero)]
    sizes = [tuple(r / SCALE for r in inverse)]
    lack = [[(EPSILON * inverse[0]) * inverse[0]]]
    alphas, betas = [], []
    for j in range(ITERS):
        newest = columns[j]
        image = pair_add(
            pair_times(newest, shifts), tuple(pltpu.roll(t, 1, 0) for t in newest)
        )
        weights = pair_sum([pair_mul(gram[k], row_of(image, k)) for k in range(j + 2)])
        dots = [pair_dot(columns[k], weights) for k in range(j + 1)]
        norm = pair_dot(image, weights)
        ready(j, columns[j], sizes[j])
        first = [pair_mul(dots[k], sizes[k]) for k in range(j + 1)]
        second = [sum(lack[k][l] * first[l][0] for l in range(j + 1)) for k in range(j + 1)]
        third = [sum(lack[k][l] * second[l] for l in range(j + 1)) for k in range(j + 1)]
        both = [pair_add(first[k], (second[k], zero)) for k in range(j + 1)]
        rest = sum(
            second[k] * second[k] - both[k][0] * (second[k] + third[k]) for k in range(j + 1)
        )
        square = pair_sum(
            [norm] + [pair_neg(pair_mul(f, f)) for f in first] + [(rest, zero)]
        )
        square = pair_mul(square, pair_mul(sizes[j], sizes[j]))
        positive = square[0] + square[1] > 0.0
        beta, inverse = root_of(tuple(jnp.where(positive, s, 0.0) for s in square))
        alphas.append(both[j][0] * sizes[j][0])
        betas.append(beta)
        columns.append(
            pair_sum(
                [image]
                + [
                    pair_neg(pair_mul(columns[k], pair_mul(both[k], sizes[k])))
                    for k in range(j + 1)
                ]
            )
        )
        sizes.append(pair_mul(sizes[j], inverse))
        for k in range(j + 1):
            lack[k].append(-third[k] * sizes[j + 1][0])
        lack.append([lack[k][j + 1] for k in range(j + 1)] + [(EPSILON * inverse[0]) * inverse[0]])
    ready(ITERS, columns[ITERS], sizes[ITERS])
    return alphas, betas


def lanczos_kernel(per_cell, rows, basis, vectors, tridiagonal, made, small, done):
    total = sum_of_rows(rows)
    lane, row = lanes(), lax.broadcasted_iota(jnp.int32, (8, 128), 0)
    gram = []
    for k in range(COUNT):
        low, high = jnp.minimum(row, k), jnp.maximum(row, k)
        place = low * COUNT - ((low * (low - 1)) >> 1) + (high - low)
        picked = (lane == place) & (row < COUNT)
        gram.append(
            tuple(
                jnp.broadcast_to(
                    jnp.sum(jnp.where(picked, t, 0.0), axis=1, keepdims=True) * per_cell, (8, 128)
                )
                for t in total
            )
        )

    def copy(j):
        return pltpu.make_async_copy(made.at[j], vectors.at[j], done.at[j])

    def ready(j, column, size):
        scaled = pair_mul(column, size)
        scaled = scaled[0] + scaled[1]
        factors = [jnp.broadcast_to(scaled[i : i + 1, :], (8, 128)) for i in range(j + 1)]
        for plane in range(8):
            for tile in range(4):
                at = slice(8 * tile, 8 * tile + 8)
                value = factors[0] * basis[0, plane, at]
                for i in range(1, j + 1):
                    value = value + factors[i] * basis[i, plane, at]
                made[j, plane, at] = value
        copy(j).start()

    alphas, betas = coefficients(gram, ready)
    for r, values in enumerate((alphas, betas)):
        table = jnp.zeros((8, 128), jnp.float32)
        for j, value in enumerate(values):
            table = jnp.where(lane == j, value, table)
        small[r : r + 1, :] = table[0:1, 0:ITERS]
    last = pltpu.make_async_copy(small, tridiagonal, done.at[COUNT])
    last.start()
    for j in range(COUNT):
        copy(j).wait()
    last.wait()


def call(kernel, out_shape, scratch=(), flops=10000, mebibytes=4, **specs):
    return pl.pallas_call(
        kernel,
        out_shape=out_shape,
        scratch_shapes=list(scratch),
        cost_estimate=pl.CostEstimate(flops=flops, bytes_accessed=flops, transcendentals=0),
        compiler_params=pltpu.CompilerParams(
            vmem_limit_bytes=mebibytes and mebibytes * 2**20
        ),
        interpret=INTERPRET,
        **specs,
    )


def to_rows(*pieces):
    return jnp.concatenate([p.reshape(-1, 128) for p in pieces])


def shards(v, p):
    f32 = jnp.float32

    def line(axis, step):
        n = lax.axis_size(axis)
        return [(i, i + step) for i in range(n) if 0 <= i + step < n]

    def exchange(to_next, to_previous, axis):
        return (
            lax.ppermute(to_next, axis, line(axis, 1)),
            lax.ppermute(to_previous, axis, line(axis, -1)),
        )

    halo = jax.ShapeDtypeStruct((9, 8, 128), f32)
    last, first = slice(24, 32), slice(0, 8)
    y_low, y_high = exchange(
        *call(edges_kernel, (halo, halo), mebibytes=1)(
            v[:, last], v[:, first], p[:, last], p[:, first]
        ),
        "py",
    )
    z_low, z_high = exchange(
        to_rows(v[3:], p[4:], y_low[4:8], y_high[4:8]),
        to_rows(v[:5], p[:4], y_low[:4], y_high[:4]),
        "pz",
    )
    blocks = (v, p, y_low, y_high, z_low, z_high)
    side = call(side_kernel, jax.ShapeDtypeStruct((88, 128), f32))(*blocks)
    side = lax.ppermute(side, "slab", [(0, 1), (1, 0)])
    n_y = lax.axis_size("py")
    n_zx = lax.axis_size("pz") * lax.axis_size("slab")
    block = [pltpu.VMEM((2, 18, 48, 128), f32)] * 5
    basis, rows = call(
        krylov_kernel,
        (jax.ShapeDtypeStruct((COUNT, 8, 32, 128), f32), jax.ShapeDtypeStruct((n_y, 128), f32)),
        block + [pltpu.VMEM((8, 32, 128), f32), pltpu.VMEM((2, 16, 48, 128), f32)],
        20000000,
        12,
    )(*blocks, side)
    rows = lax.all_to_all(rows, "py", 0, 0, tiled=True)
    rows = call(rows_kernel, jax.ShapeDtypeStruct((n_zx, 128), f32))(rows)
    rows = lax.all_to_all(rows, ("pz", "slab"), 0, 0, tiled=True)
    per_cell = 1.0 / (v.size * n_y * n_zx)
    return call(
        functools.partial(lanczos_kernel, per_cell),
        (
            jax.ShapeDtypeStruct((COUNT, 8, 32, 128), f32),
            jax.ShapeDtypeStruct((2, ITERS), f32),
        ),
        [
            pltpu.VMEM((COUNT, 8, 32, 128), f32),
            pltpu.VMEM((2, ITERS), f32),
            pltpu.SemaphoreType.DMA((COUNT + 1,)),
        ],
        flops=20000000,
        out_specs=(pl.BlockSpec(memory_space=pl.ANY),) * 2,
    )(rows, basis)


def solution(mesh):
    in_specs = (P("pz", "py", "slab"), P("pz", "py", "slab"))
    out_specs = (P(None, "pz", "py", "slab"), P())
    return jax.shard_map(shards, mesh=mesh, in_specs=in_specs, out_specs=out_specs, check_vma=False)
```
